128 devices in a mesh: dp: 32 (over z, y, x_lo), tensor: 4 (over x_hi, core).
Axes of the slice: x: 4 (x_hi: 2, x_lo: 2; x = x_hi * 2 + x_lo), y: 4, z: 4, core: 2. Of those that a mesh axis runs over, the one named last changes fastest.
Arguments:
- patches: bfloat16 [32768, 1280], P('dp'), may hold values from -27 to 27
- norm_gain: float32 [1280], replicated, may hold values from 0.1 to 1.9
- norm_bias: float32 [1280], replicated, may hold values from -3 to 3
- first_weight: bfloat16 [5120, 5120], P(None, 'tensor'), may hold values from -0.078125 to 0.078125
- first_bias: float32 [5120], P('tensor'), may hold values from -3 to 3
- second_weight: bfloat16 [5120, 8192], P('tensor', 'dp'), may hold values from -0.078125 to 0.078125
- second_bias: float32 [8192], P('tensor'), may hold values from -2 to 2
- text_embeds: bfloat16 [16384, 8192], P('dp', 'tensor'), may hold values from -36 to 36
- final_gain: float32 [8192], P('tensor'), may hold values from 0.1 to 1.9
- image_grids: int32 [32, 4, 2], replicated, may hold values from 2 to 8, as said below
- routing: int32 [32, 4], replicated, may hold values from 0 to 3, each once within a row
Outputs:
- embeddings: bfloat16 [16384, 8192], P('dp', 'tensor')
- normed: bfloat16 [16384, 8192], P('dp', 'tensor')
The draws below stay inside these ranges and needn't reach their ends.
Inputs may be any that keep to these rules, and one draw needn't show every extreme that they name: `image_grids`: each image is a grid of 3 to 8 rows by 2 to 8 columns of merged tokens; in every draw some image is 8 by 8. `routing`: each row names every offset 0 to 3 once.
All inputs are finite; a program needn't handle non-finite values.
Results may differ from the reference program's by a relative error of at most 0.006.
Values may be sent and summed in bfloat16 or wider, within the bound.
A program may use at most 128 MiB of HBM per device.

```python
import jax
import jax.numpy as jnp
from jax import lax

D_VIT = 1280
D = 8192
D_MERGE = 5120
BLOCKS = 4
SLOTS = 256
CAP = 64
SEQ = 512
SHARDS = 32
PATCHES = 32768
TOTAL_SEQ = 16384
N_TENSOR = 4


def draw_patches(key, part):
    keys = jax.random.split(jax.random.fold_in(key, 11), 3)
    row_scale = jnp.exp(jax.random.uniform(keys[1], (PATCHES, 1), jnp.float32, jnp.log(0.5), jnp.log(5.0)))
    row_offset = jax.random.uniform(keys[2], (PATCHES, 1), jnp.float32, -1.0, 1.0)
    base = jax.random.normal(keys[0], (PATCHES, D_VIT), jnp.float32)
    base = jnp.clip(base, -5.0, 5.0)
    return (base * row_scale + row_offset).astype(jnp.bfloat16)


def draw_text_embeds(key, part):
    keys = jax.random.split(jax.random.fold_in(key, 23), 3)
    column_ids = jnp.arange(D, dtype=jnp.float32)
    column_scale = 0.6 * jnp.power(3.0, column_ids / (D - 1)) * jax.random.uniform(keys[1], (D,), jnp.float32, 0.7, 1.3)
    row_scale = jnp.exp(jax.random.uniform(keys[2], (TOTAL_SEQ, 1), jnp.float32, jnp.log(0.3), jnp.log(3.0)))
    base = jax.random.normal(keys[0], (TOTAL_SEQ, D), jnp.float32)
    base = jnp.clip(base, -5.0, 5.0)
    return (base * row_scale * column_scale[None, :]).astype(jnp.bfloat16)


def draw_image_grids(key, part):
    keys = jax.random.split(jax.random.fold_in(key, 37), 4)
    grid_rows = jax.random.randint(keys[0], (SHARDS, BLOCKS), 3, 9)
    grid_columns = jax.random.randint(keys[1], (SHARDS, BLOCKS), 2, CAP // 8 + 1)
    full_shard = jax.random.randint(keys[2], (), 0, SHARDS)
    full_block = jax.random.randint(keys[3], (), 0, BLOCKS)
    shard_ids = jnp.arange(SHARDS, dtype=jnp.int32)[:, None]
    block_ids = jnp.arange(BLOCKS, dtype=jnp.int32)[None, :]
    target = (shard_ids == full_shard) & (block_ids == full_block)
    grid_rows = jnp.where(target, 8, grid_rows)
    grid_columns = jnp.where(target, CAP // 8, grid_columns)
    return jnp.stack([grid_rows, grid_columns], axis=-1).astype(jnp.int32)


def levels(own_key, shape, pieces, smallest, largest):
    def one(dim, shards_of):
        steps = jax.random.uniform(jax.random.fold_in(jax.random.fold_in(own_key, 6), dim), (shards_of,), jnp.float32, smallest / len(pieces), largest / len(pieces))
        return jnp.repeat(jnp.exp(steps), shape[dim] // shards_of).reshape((-1,) + (1,) * (len(shape) - dim - 1))

    loudness = one(*pieces[0])
    for cut in pieces[1:]:
        loudness = loudness * one(*cut)
    return loudness


def normal_values(own_key, shape, width, most, cuts=(), kind=jnp.bfloat16):
    level = levels(own_key, shape, cuts, -0.22, 0.18) if cuts else 1.0
    drawn = jax.random.normal(own_key, shape, jnp.float32) * width * level
    return jnp.minimum(jnp.maximum(drawn, -most), most).astype(kind)


def setup_inputs(seed: int = 0) -> dict:
    seeds = jax.random.split(jax.random.key(seed), 12)
    patches = draw_patches(jax.random.fold_in(seeds[11], 71), 0)
    norm_gain = jnp.clip(1.0 + 0.18 * jax.random.normal(seeds[1], (D_VIT,), jnp.float32), 0.1, 1.9)
    norm_bias = normal_values(seeds[2], (D_VIT,), 0.5, 3.0, (), jnp.float32)
    first_weight = normal_values(seeds[3], (D_MERGE, D_MERGE), D_MERGE ** -0.5, 0.078125, ((1, 4),))
    first_bias = normal_values(seeds[4], (D_MERGE,), 0.5, 3.0, ((0, 4),), jnp.float32)
    second_weight = normal_values(seeds[5], (D_MERGE, D), D_MERGE ** -0.5, 0.078125, ((0, 4), (1, 32)))
    second_bias = normal_values(seeds[6], (D,), 0.3, 2.0, ((0, 4),), jnp.float32)
    text_embeds = draw_text_embeds(jax.random.fold_in(seeds[11], 71), 0)
    final_gain = jnp.clip(1.0 + 0.18 * jax.random.normal(seeds[8], (D,), jnp.float32), 0.1, 1.9)
    image_grids = draw_image_grids(jax.random.fold_in(seeds[11], 71), 0)
    routing = jax.vmap(lambda own: jax.random.permutation(own, BLOCKS))(jax.random.split(seeds[10], SHARDS)).reshape((SHARDS, BLOCKS)).astype(jnp.int32)
    return {"patches": patches, "norm_gain": norm_gain, "norm_bias": norm_bias, "first_weight": first_weight, "first_bias": first_bias, "second_weight": second_weight, "second_bias": second_bias, "text_embeds": text_embeds, "final_gain": final_gain, "image_grids": image_grids, "routing": routing}


def reference(patches, norm_gain, norm_bias, first_weight, first_bias, second_weight, second_bias, text_embeds, final_gain, image_grids, routing):
    patch_values = patches.astype(jnp.float32)
    centered = patch_values - lax.optimization_barrier(jnp.mean(patch_values, axis=-1, keepdims=True))
    variance = lax.optimization_barrier(jnp.mean(centered * centered, axis=-1, keepdims=True))
    normed_patches = centered * lax.rsqrt(variance + 1e-06) * norm_gain + norm_bias
    merged = normed_patches.reshape(-1, D_MERGE).astype(jnp.bfloat16)
    hidden = jax.nn.gelu(jnp.dot(merged, first_weight, preferred_element_type=jnp.float32) + first_bias, approximate=False).astype(jnp.bfloat16)
    group_width = D_MERGE // N_TENSOR
    summed = jnp.zeros((hidden.shape[0], D), jnp.float32)
    for group in range(N_TENSOR):
        partial_value = jnp.dot(hidden[:, group * group_width:(group + 1) * group_width], second_weight[group * group_width:(group + 1) * group_width], preferred_element_type=jnp.float32).astype(jnp.bfloat16)
        partial_value = lax.optimization_barrier(partial_value)
        summed = summed + partial_value.astype(jnp.float32)
    projected = (summed + second_bias).astype(jnp.bfloat16)
    counts_all = (image_grids[:, :, 0] * image_grids[:, :, 1]).astype(jnp.int32)
    shard_ids = jnp.arange(SHARDS, dtype=jnp.int32)[:, None]
    stride_ids = jnp.arange(BLOCKS, dtype=jnp.int32)[None, :]
    source_shard = ((shard_ids - stride_ids) % SHARDS).astype(jnp.int32)
    source_routing = routing[source_shard]
    block_ids = jnp.arange(BLOCKS, dtype=jnp.int32)[None, None, :]
    chosen = lax.optimization_barrier(jnp.sum(jnp.where(source_routing == stride_ids[:, :, None], block_ids, 0), axis=-1)).astype(jnp.int32)
    lengths = counts_all[source_shard, chosen]
    starts = (jnp.cumsum(lengths, axis=1) - lengths).astype(jnp.int32)
    totals = lax.optimization_barrier(jnp.sum(lengths, axis=1))
    position = jnp.arange(SEQ, dtype=jnp.int32)[None, :]
    which = lax.optimization_barrier(jnp.sum((position[:, :, None] >= starts[:, None, 1:]).astype(jnp.int32), axis=-1)).astype(jnp.int32)
    start_at = jnp.take_along_axis(starts, which, axis=1)
    source_at = jnp.take_along_axis(source_shard, which, axis=1)
    chosen_at = jnp.take_along_axis(chosen, which, axis=1)
    valid = position < totals[:, None]
    row_index = jnp.where(valid, source_at * SLOTS + chosen_at * CAP + position - start_at, 0).astype(jnp.int32)
    image_rows = jnp.take(projected, row_index.reshape(-1), axis=0).reshape(SHARDS, SEQ, D)
    text_rows = text_embeds.reshape(SHARDS, SEQ, D)
    embeddings = jnp.where(valid[:, :, None], image_rows, text_rows).reshape(SHARDS * SEQ, D)
    embed_values = embeddings.astype(jnp.float32)
    mean_square = lax.optimization_barrier(jnp.mean(embed_values * embed_values, axis=-1, keepdims=True))
    normed = (embed_values * lax.rsqrt(mean_square + 1e-06) * final_gain).astype(jnp.bfloat16)
    return (embeddings, normed)
```

```python
import functools

import jax
import jax.numpy as jnp
from jax import lax
from jax.experimental import pallas as pl
from jax.experimental.pallas import tpu as pltpu
from jax.sharding import PartitionSpec as P

MESH = pl.DeviceIdType.MESH
F32 = jnp.float32
BF16 = jnp.bfloat16
SHARDS = 32
CAP = 64
D = 8192
CH = 256
NCH = 5
HEAD = 192
SQRT_HALF = 0.7071067811865476


def wait_for(ref, sem):
    pltpu.make_async_copy(ref, ref, sem).wait()


def send(src, dst, send_sem, recv_sem, device):
    pltpu.make_async_remote_copy(
        src_ref=src,
        dst_ref=dst,
        send_sem=send_sem,
        recv_sem=recv_sem,
        device_id=device,
        device_id_type=MESH,
    ).start()


def row_squares(values):
    ones = jnp.ones((8, values.shape[1]), F32)
    return lax.dot_general(
        ones,
        values,
        (((1,), (1,)), ((), ())),
        precision=lax.Precision.HIGHEST,
        preferred_element_type=F32,
    )


def merge_kernel(
    routing_ref,
    pat_hbm,
    gain_ref,
    nbias_ref,
    w1_hbm,
    b1_ref,
    w2_hbm,
    b2_ref,
    text_hbm,
    img_out,
    sums_out,
    pat,
    w1,
    nbuf,
    mer,
    hid,
    wbuf,
    text,
    dsend,
    drecv,
    xsend,
    xrecv,
    fbuf,
    obuf,
    img,
    sbuf,
    lsem,
    s0,
    s_swap,
    s_w,
    s_h,
    s_d,
    s_x,
    s_i,
    s_s,
    r_om,
    r_op,
    r_p,
    r_fm,
    r_fp,
    r_pm,
    r_pp,
    r_p2,
    r_h1,
    r_h2,
    r_h3,
    r_d,
    r_x,
    r_i,
    r_s,
):
    d = lax.axis_index("dp")
    t = lax.axis_index("tensor")
    z = lax.div(d, 8)
    y = lax.rem(lax.div(d, 2), 4)
    xl = lax.rem(d, 2)
    xh = lax.div(t, 2)
    c = lax.rem(t, 2)
    zp = lax.rem(z + 1, 4)
    zm = lax.rem(z + 3, 4)
    zo = lax.rem(z + 2, 4)
    yb = y + 1 - 2 * lax.rem(y, 2)
    q = xl + xh - 2 * xl * xh
    dev_zp = (zp * 8 + y * 2 + xl, t)
    dev_zm = (zm * 8 + y * 2 + xl, t)
    dev_ya = (z * 8 + (3 - y) * 2 + xl, t)
    dev_yb = (z * 8 + yb * 2 + xl, t)
    dev_x = (z * 8 + y * 2 + 1 - xl, t)
    dev_cut = (z * 8 + y * 2 + 1 - xl, (1 - xh) * 2 + c)
    dev_core = (d, xh * 2 + 1 - c)

    pltpu.make_async_copy(pat_hbm, pat, lsem.at[NCH]).start()

    def w1_copy(n):
        return pltpu.make_async_copy(
            w1_hbm.at[:, pl.ds(n * CH, CH)], w1.at[n], lsem.at[n]
        )

    w1_copy(0).start()

    @pl.when(xh == 0)
    def _():
        for kc in range(NCH):
            pltpu.make_async_copy(
                w2_hbm.at[pl.ds(kc * CH, CH)], wbuf.at[z * 2, kc], s0.at[kc]
            ).start()

    for n in range(1, NCH):
        w1_copy(n).start()
    pltpu.make_async_copy(text_hbm, text, lsem.at[NCH + 1]).start()

    barrier = pltpu.get_barrier_semaphore()
    base = d - lax.rem(d, 4)

    def greet(device):
        pl.semaphore_signal(barrier, inc=1, device_id=device, device_id_type=MESH)

    for o in range(-4, 8):
        other = lax.rem(base + o + SHARDS, SHARDS)

        @pl.when(other != d)
        def _():
            greet((other, t))

    greet(dev_zp)
    greet(dev_zm)
    greet(dev_cut)
    for i in range(1, 4):
        greet((d, lax.rem(t + i, 4)))
    pl.semaphore_wait(barrier, 17)

    def own_send(kc):
        block = wbuf.at[z * 2, kc]
        wait_for(block, s0.at[kc])
        send(block, block, s_w, r_om.at[kc], dev_zp)
        send(block, block, s_w, r_op.at[kc], dev_zm)
        send(block, wbuf.at[z * 2 + 1, kc], s_w, r_p.at[kc], dev_ya)

    @pl.when(xh == 1)
    def _():
        for kc in range(NCH):
            send(
                w2_hbm.at[pl.ds(kc * CH, CH)],
                wbuf.at[z * 2, kc],
                s_swap,
                s0.at[kc],
                dev_x,
            )

    @pl.when(xh == 0)
    def _():
        for kc in range(NCH):
            own_send(kc)

    wait_for(pat, lsem.at[NCH])
    gain = gain_ref[...]
    nbias = nbias_ref[...]
    width = pat.shape[1]

    def norm_step(step, carry):
        slot = lax.div(step, 4)
        part = lax.rem(step, 4)
        values = jnp.zeros((64, width), F32)
        for b in range(4):
            start = pl.multiple_of(b * (4 * CAP) + part * 64, 64)
            chosen = (routing_ref[d, b] == slot).astype(F32)
            values = values + pat[pl.ds(start, 64), :].astype(F32) * chosen
        centered = values - jnp.mean(values, axis=-1, keepdims=True)
        variance = jnp.mean(centered * centered, axis=-1, keepdims=True)
        normed = centered * lax.rsqrt(variance + 1e-06) * gain + nbias
        row = pl.multiple_of(step * 16, 16)
        for i in range(width // 128):
            nbuf[i] = normed[:, i * 128 : (i + 1) * 128]
        for j in range(4):
            for i in range(width // 128):
                mer[pl.ds(row, 16), j * width + i * 128 : j * width + (i + 1) * 128] = (
                    nbuf[i, pl.ds(j, 16, stride=4), :].astype(BF16)
                )
        return carry

    lax.fori_loop(0, 16, norm_step, 0)

    def hidden_step(n, carry):
        wait_for(w1.at[n], lsem.at[n])
        value = jnp.dot(mer[...], w1[n], preferred_element_type=F32)
        value = value + b1_ref[pl.ds(n, 1), :]
        value = 0.5 * value * (1.0 + lax.erf(value * SQRT_HALF))
        hid[0, n] = value.astype(BF16)
        send(hid.at[0, n], hid.at[1, n], s_h, r_h1.at[n], dev_x)
        send(hid.at[0, n], hid.at[2, n], s_h, r_h2.at[n], dev_yb)

        @pl.when((xh == 1) & (lax.rem(n, 2) == 0))
        def _():
            own_send(lax.div(n, 2))

        return carry

    lax.fori_loop(0, NCH, hidden_step, 0)

    def relay_far(kc, carry):
        @pl.when((xh == 1) & (kc < 2))
        def _():
            own_send(kc + 3)

        wait_for(wbuf.at[zm * 2, kc], r_om.at[kc])
        upper = wbuf.at[zm * 2, kc, pl.ds(0, CH // 2)]
        send(upper, upper, s_w, r_fm.at[kc], dev_zp)
        wait_for(wbuf.at[zp * 2, kc], r_op.at[kc])
        under = wbuf.at[zp * 2, kc, pl.ds(CH // 2, CH // 2)]
        send(under, under, s_w, r_fp.at[kc], dev_zm)
        return carry

    lax.fori_loop(0, NCH, relay_far, 0)

    def relay_pair(kc, carry):
        block = wbuf.at[z * 2 + 1, kc]
        wait_for(block, r_p.at[kc])
        send(block, block, s_w, r_pm, dev_zp)
        send(block, block, s_w, r_pp, dev_zm)
        return carry

    lax.fori_loop(0, NCH, relay_pair, 0)

    wait_for(text, lsem.at[NCH + 1])

    def text_step(i, carry):
        rows = pl.ds(pl.multiple_of(i * CH, CH), CH)
        total = jnp.zeros((CH, CH), F32)
        for j in range(8):
            values = text[rows, j * CH : (j + 1) * CH].astype(F32)
            total = total + values * values
        sbuf[t, :, rows] = row_squares(total)
        return carry

    lax.fori_loop(0, 2, text_step, 0)

    def relay_rows(n, carry):
        wait_for(hid.at[1, n], r_h1.at[n])
        send(
            hid.at[1, n, pl.ds(0, HEAD)],
            hid.at[3, n, pl.ds(0, HEAD)],
            s_h,
            r_h3,
            dev_yb,
        )
        wait_for(hid.at[2, n], r_h2.at[n])
        send(
            hid.at[2, n, pl.ds(HEAD, CH - HEAD)],
            hid.at[3, n, pl.ds(HEAD, CH - HEAD)],
            s_h,
            r_h3,
            dev_x,
        )
        wait_for(wbuf.at[zo * 2, n, pl.ds(0, CH // 2)], r_fm.at[n])
        wait_for(wbuf.at[zo * 2, n, pl.ds(CH // 2, CH // 2)], r_fp.at[n])
        send(wbuf.at[zo * 2, n], wbuf.at[zo * 2 + 1, n], s_w, r_p2, dev_ya)
        return carry

    lax.fori_loop(0, NCH, relay_rows, 0)
    wait_for(hid.at[3], r_h3)

    def tile(r, group, p):
        total = jnp.dot(hid[r, 0], wbuf[group * 2 + p, 0], preferred_element_type=F32)
        for n in range(1, NCH):
            total = total + jnp.dot(
                hid[r, n], wbuf[group * 2 + p, n], preferred_element_type=F32
            )
        return total

    other = (1 - xh) * 2
    mine = xh * 2

    def to_core(half, p, group):
        def step(r, carry):
            dsend[half, p, r] = tile(r, group, p).astype(BF16)
            send(
                dsend.at[half, p, r],
                drecv.at[half, p, r],
                s_d,
                r_d.at[half * 8 + p * 4 + r],
                dev_core,
            )
            return carry

        lax.fori_loop(0, 4, step, 0)

    def across(p):
        def step(r, carry):
            value = tile(r, other + c, p)
            wait_for(drecv.at[0, p, r], r_d.at[p * 4 + r])
            value = value + drecv[0, p, r].astype(F32)
            xsend[p, r] = value.astype(BF16)
            there = r + 1 - 2 * lax.rem(r, 2)
            send(
                xsend.at[p, r], xrecv.at[p, there], s_x, r_x.at[p * 4 + there], dev_cut
            )
            return carry

        lax.fori_loop(0, 4, step, 0)

    def keep(p):
        column = pl.multiple_of((y + p * (3 - 2 * y)) * 512 + q * CH, CH)
        bias = b2_ref[:, pl.ds(column, CH)]

        def step(r, carry):
            value = tile(r, mine + c, p)
            wait_for(drecv.at[1, p, r], r_d.at[8 + p * 4 + r])
            fbuf[p, r] = value + drecv[1, p, r].astype(F32) + bias
            return carry

        lax.fori_loop(0, 4, step, 0)

    to_core(0, 0, other + 1 - c)
    across(0)
    wait_for(wbuf.at[zm * 2 + 1], r_pm)
    wait_for(wbuf.at[zp * 2 + 1], r_pp)
    wait_for(wbuf.at[zo * 2 + 1], r_p2)
    to_core(0, 1, other + 1 - c)
    across(1)
    to_core(1, 0, mine + 1 - c)
    to_core(1, 1, mine + 1 - c)
    keep(0)
    keep(1)

    def target(r, k):
        row_y = y + lax.div(r, 2) * (yb - y)
        row_x = xl + lax.rem(r, 2) * (1 - 2 * xl)
        return lax.rem(z * 8 + row_y * 2 + row_x + k, SHARDS)

    def pieces(p, r, k):
        rows = pl.ds(k * CAP, CAP)
        column = (y + p * (3 - 2 * y)) * 2 + q
        return obuf.at[p, r, rows], img.at[column, rows]

    for p in range(2):

        def finish(r, carry):
            wait_for(xrecv.at[p, r], r_x.at[p * 4 + r])
            obuf[p, r] = (fbuf[p, r] + xrecv[p, r].astype(F32)).astype(BF16)
            for k in range(4):
                e = target(r, k)
                src, dst = pieces(p, r, k)

                @pl.when(e == d)
                def _():
                    pltpu.make_async_copy(src, dst, r_i).start()

                @pl.when(e != d)
                def _():
                    send(src, dst, s_i.at[p * 16 + r * 4 + k], r_i, (e, t))

            return carry

        lax.fori_loop(0, 4, finish, 0)

    wait_for(img, r_i)
    img_copy = pltpu.make_async_copy(img, img_out, lsem.at[0])
    img_copy.start()
    total = jnp.zeros((CH, CH), F32)
    for b in range(8):
        values = img[b].astype(F32)
        total = total + values * values
    sbuf[t, :, pl.ds(512, CH)] = row_squares(total)
    for i in range(1, 4):
        send(
            sbuf.at[t],
            sbuf.at[t],
            s_s.at[i - 1],
            r_s.at[i - 1],
            (d, lax.rem(t + i, 4)),
        )
    for i in range(1, 4):
        wait_for(sbuf.at[lax.rem(t + 4 - i, 4)], r_s.at[i - 1])
    sums_copy = pltpu.make_async_copy(sbuf, sums_out, lsem.at[1])
    sums_copy.start()

    wait_for(wbuf.at[pl.ds(0, 7)], s_w)

    @pl.when(xh == 1)
    def _():
        wait_for(wbuf.at[0], s_swap)

    wait_for(hid.at[pl.ds(0, 3)], s_h)
    wait_for(dsend, s_d)
    wait_for(xsend, s_x)
    for p in range(2):

        def drain(r, carry):
            for k in range(4):
                src, _unused = pieces(p, r, k)

                @pl.when(target(r, k) != d)
                def _():
                    wait_for(src, s_i.at[p * 16 + r * 4 + k])

            return carry

        lax.fori_loop(0, 4, drain, 0)
    for i in range(1, 4):
        wait_for(sbuf.at[t], s_s.at[i - 1])
    img_copy.wait()
    sums_copy.wait()


def splice_kernel(
    grids_ref, routing_ref, text_ref, img_ref, sums_ref, gain_ref, emb_ref, out_ref
):
    d = lax.axis_index("dp")
    g = pl.program_id(0)
    rows = text_ref.shape[0]
    starts = []
    total = jnp.int32(0)
    for k in range(4):
        s = lax.rem(d + SHARDS - k, SHARDS)
        count = jnp.int32(0)
        for b in range(4):
            size = grids_ref[s, 2 * b] * grids_ref[s, 2 * b + 1]
            count = count + jnp.where(routing_ref[s, b] == k, size, 0)
        starts.append(total)
        total = total + count
    position = g * rows + lax.broadcasted_iota(jnp.int32, (rows, 1), 0)
    source = position
    for k in range(1, 4):
        begin = jnp.where(position >= starts[k], k * CAP - starts[k], 0)
        if k > 1:
            begin = begin - jnp.where(
                position >= starts[k], (k - 1) * CAP - starts[k - 1], 0
            )
        source = source + begin
    live = position < total
    sums = sums_ref[0] + sums_ref[1] + sums_ref[2] + sums_ref[3]
    sums = sums[0:1, :]
    index = jnp.where(live, 512 + source, position)
    lanes = lax.broadcasted_iota(jnp.int32, (rows, sums.shape[1]), 1)
    square = jnp.sum(jnp.where(lanes == index, sums, 0.0), axis=-1, keepdims=True)
    scale = lax.rsqrt(square / D + 1e-06)
    picks = jnp.where(
        lax.broadcasted_iota(jnp.int32, (rows, 4 * CAP), 1) == source, 1.0, 0.0
    ).astype(BF16)
    blocks = img_ref.shape[0]

    @pl.when(g * rows < 4 * CAP)
    def _():
        for b in range(blocks):
            cols = slice(b * CH, (b + 1) * CH)
            taken = jnp.dot(picks, img_ref[b], preferred_element_type=F32)
            value = jnp.where(live, taken, text_ref[:, cols].astype(F32))
            emb_ref[:, cols] = value.astype(BF16)
            out_ref[:, cols] = (value * scale * gain_ref[:, cols]).astype(BF16)

    @pl.when(g * rows >= 4 * CAP)
    def _():
        for b in range(blocks):
            cols = slice(b * CH, (b + 1) * CH)
            value = text_ref[:, cols].astype(F32)
            emb_ref[:, cols] = text_ref[:, cols]
            out_ref[:, cols] = (value * scale * gain_ref[:, cols]).astype(BF16)


def per_device(
    patches,
    norm_gain,
    norm_bias,
    first_weight,
    first_bias,
    second_weight,
    second_bias,
    text_embeds,
    final_gain,
    image_grids,
    routing,
):
    seq, features = text_embeds.shape
    width = patches.shape[1]
    hbm = pl.BlockSpec(memory_space=pl.ANY)
    vmem = pl.BlockSpec(memory_space=pltpu.VMEM)
    smem = pl.BlockSpec(memory_space=pltpu.SMEM)
    dma = pltpu.SemaphoreType.DMA
    img, sums = pl.pallas_call(
        merge_kernel,
        out_shape=(
            jax.ShapeDtypeStruct((8, CH, CH), BF16),
            jax.ShapeDtypeStruct((4, 8, seq + CH), F32),
        ),
        in_specs=[smem, hbm, vmem, vmem, hbm, vmem, hbm, vmem, hbm],
        out_specs=(hbm, hbm),
        scratch_shapes=[
            pltpu.VMEM(patches.shape, BF16),
            pltpu.VMEM((NCH, first_weight.shape[0], CH), BF16),
            pltpu.VMEM((width // 128, 64, 128), F32),
            pltpu.VMEM((CH, 4 * width), BF16),
            pltpu.VMEM((4, NCH, CH, CH), BF16),
            pltpu.VMEM((8, NCH, CH, CH), BF16),
            pltpu.VMEM((seq, features), BF16),
            pltpu.VMEM((2, 2, 4, CH, CH), BF16),
            pltpu.VMEM((2, 2, 4, CH, CH), BF16),
            pltpu.VMEM((2, 4, CH, CH), BF16),
            pltpu.VMEM((2, 4, CH, CH), BF16),
            pltpu.VMEM((2, 4, CH, CH), F32),
            pltpu.VMEM((2, 4, CH, CH), BF16),
            pltpu.VMEM((8, CH, CH), BF16),
            pltpu.VMEM((4, 8, seq + CH), F32),
            dma((NCH + 2,)),
            dma((NCH,)),
            dma,
            dma,
            dma,
            dma,
            dma,
            dma((32,)),
            dma((3,)),
            dma((NCH,)),
            dma((NCH,)),
            dma((NCH,)),
            dma((NCH,)),
            dma((NCH,)),
            dma,
            dma,
            dma,
            dma((NCH,)),
            dma((NCH,)),
            dma,
            dma((16,)),
            dma((8,)),
            dma,
            dma((3,)),
        ],
        compiler_params=pltpu.CompilerParams(
            collective_id=0, has_side_effects=True, vmem_limit_bytes=60 * 1024 * 1024
        ),
        name="merge",
    )(
        routing,
        patches,
        norm_gain.reshape(1, -1),
        norm_bias.reshape(1, -1),
        first_weight,
        first_bias.reshape(NCH, CH),
        second_weight,
        second_bias.reshape(1, -1),
        text_embeds,
    )
    rows = 128
    return pl.pallas_call(
        splice_kernel,
        grid=(seq // rows,),
        out_shape=(
            jax.ShapeDtypeStruct((seq, features), BF16),
            jax.ShapeDtypeStruct((seq, features), BF16),
        ),
        in_specs=[
            smem,
            smem,
            pl.BlockSpec((rows, features), lambda g: (g, 0)),
            vmem,
            vmem,
            vmem,
        ],
        out_specs=(
            pl.BlockSpec((rows, features), lambda g: (g, 0)),
            pl.BlockSpec((rows, features), lambda g: (g, 0)),
        ),
        name="splice",
    )(
        image_grids.reshape(SHARDS, -1),
        routing,
        text_embeds,
        img,
        sums,
        final_gain.reshape(1, -1),
    )


def solution(mesh):
    placed = (
        P("dp", None),
        P(),
        P(),
        P(None, "tensor"),
        P("tensor"),
        P("tensor", "dp"),
        P("tensor"),
        P("dp", "tensor"),
        P("tensor"),
        P(),
        P(),
    )
    return jax.shard_map(
        per_device,
        mesh=mesh,
        in_specs=placed,
        out_specs=(P("dp", "tensor"), P("dp", "tensor")),
        check_vma=False,
    )
```

```python
import functools

import jax
import jax.numpy as jnp
from jax import lax
from jax.experimental import pallas as pl
from jax.experimental.pallas import tpu as pltpu
from jax.sharding import PartitionSpec as P

MESH = pl.DeviceIdType.MESH
F32 = jnp.float32
BF16 = jnp.bfloat16
SHARDS = 32
CAP = 64
D = 8192
CH = 256
NCH = 5
HEADS = (128, 208)
SQRT_HALF = 0.7071067811865476


def wait_for(ref, sem):
    pltpu.make_async_copy(ref, ref, sem).wait()


def send(src, dst, send_sem, recv_sem, device):
    pltpu.make_async_remote_copy(
        src_ref=src,
        dst_ref=dst,
        send_sem=send_sem,
        recv_sem=recv_sem,
        device_id=device,
        device_id_type=MESH,
    ).start()


def loop(name, count, step):
    with jax.named_scope(name):
        lax.fori_loop(0, count, step, 0)


def row_squares(values):
    ones = jnp.ones((8, values.shape[1]), F32)
    return lax.dot_general(
        ones,
        values,
        (((1,), (1,)), ((), ())),
        precision=lax.Precision.HIGHEST,
        preferred_element_type=F32,
    )


def merge_kernel(
    routing_ref,
    pat_hbm,
    gain_ref,
    nbias_ref,
    w1_hbm,
    b1_ref,
    w2_hbm,
    b2_ref,
    text_hbm,
    img_out,
    sums_out,
    pat,
    w1,
    nbuf,
    mer,
    hid,
    wbuf,
    stage,
    text,
    dsend,
    drecv,
    xsend,
    xrecv,
    fbuf,
    obuf,
    img,
    sbuf,
    lsem,
    s0,
    s_stage,
    s_swap,
    s_w,
    s_h,
    s_d,
    s_x,
    s_i,
    s_s,
    r_om,
    r_op,
    r_p,
    r_fm,
    r_fp,
    r_pm,
    r_pp,
    r_p2,
    r_h1,
    r_h2,
    r_h3,
    r_d,
    r_x,
    r_i,
    r_s,
):
    d = lax.axis_index("dp")
    t = lax.axis_index("tensor")
    z = lax.div(d, 8)
    y = lax.rem(lax.div(d, 2), 4)
    xl = lax.rem(d, 2)
    xh = lax.div(t, 2)
    c = lax.rem(t, 2)
    zp = lax.rem(z + 1, 4)
    zm = lax.rem(z + 3, 4)
    zo = lax.rem(z + 2, 4)
    yb = y + 1 - 2 * lax.rem(y, 2)
    q = xl + xh - 2 * xl * xh
    dev_zp = (zp * 8 + y * 2 + xl, t)
    dev_zm = (zm * 8 + y * 2 + xl, t)
    dev_ya = (z * 8 + (3 - y) * 2 + xl, t)
    dev_yb = (z * 8 + yb * 2 + xl, t)
    dev_x = (z * 8 + y * 2 + 1 - xl, t)
    dev_cut = (z * 8 + y * 2 + 1 - xl, (1 - xh) * 2 + c)
    dev_core = (d, xh * 2 + 1 - c)

    @pl.when(xh == 0)
    def _():
        pltpu.make_async_copy(w2_hbm, wbuf.at[z * 2], s_stage).start()

    @pl.when(xh == 1)
    def _():
        pltpu.make_async_copy(w2_hbm, stage, s_stage).start()

    pltpu.make_async_copy(pat_hbm, pat, lsem.at[NCH]).start()

    barrier = pltpu.get_barrier_semaphore()
    base = d - lax.rem(d, 4)

    def greet(device):
        pl.semaphore_signal(barrier, inc=1, device_id=device, device_id_type=MESH)

    for o in range(-4, 8):
        other = lax.rem(base + o + SHARDS, SHARDS)

        @pl.when(other != d)
        def _():
            greet((other, t))

    greet(dev_zp)
    greet(dev_zm)
    greet(dev_cut)
    for i in range(1, 4):
        greet((d, lax.rem(t + i, 4)))

    width = pat.shape[1]
    gain = gain_ref[...].reshape(1, width)
    nbias = nbias_ref[...].reshape(1, width)

    def norm_pair(pair, carry):
        for u in range(2):
            norm_step(pair * 2 + u, nbuf.at[u])
        return carry

    def norm_step(step, nbuf):
        slot = lax.div(step, 4)
        part = lax.rem(step, 4)
        values = jnp.zeros((64, width), BF16)
        for b in range(4):
            start = pl.multiple_of(b * (4 * CAP) + part * 64, 64)
            chosen = (routing_ref[b, d] == slot).astype(F32).astype(BF16)
            values = values + pat[pl.ds(start, 64), :] * chosen
        values = values.astype(F32)
        centered = values - jnp.mean(values, axis=-1, keepdims=True)
        variance = jnp.mean(centered * centered, axis=-1, keepdims=True)
        normed = centered * lax.rsqrt(variance + 1e-06) * gain + nbias
        row = pl.multiple_of(step * 16, 16)
        for i in range(width // 128):
            nbuf[i] = normed[:, i * 128 : (i + 1) * 128]
        for j in range(4):
            for i in range(width // 128):
                mer[pl.ds(row, 16), j * width + i * 128 : j * width + (i + 1) * 128] = (
                    nbuf[i, pl.ds(j, 16, stride=4), :].astype(BF16)
                )

    with jax.named_scope("patches_in"):
        wait_for(pat, lsem.at[NCH])
    for n in range(NCH):
        pltpu.make_async_copy(
            w1_hbm.at[:, pl.ds(n * CH, CH)], w1.at[n], lsem.at[n]
        ).start()
    with jax.named_scope("norm_first"):
        lax.fori_loop(0, 2, norm_pair, 0)
    with jax.named_scope("greeting"):
        pl.semaphore_wait(barrier, 17)

    def own_send(kc):
        block = wbuf.at[z * 2, kc]
        send(block, block, s_w, r_om.at[kc], dev_zp)
        send(block, block, s_w, r_op.at[kc], dev_zm)
        send(block, wbuf.at[z * 2 + 1, kc], s_w, r_p.at[kc], dev_ya)

    with jax.named_scope("second_in"):
        wait_for(stage, s_stage)

    def swapped_send(kc):
        with jax.named_scope("swapped"):
            wait_for(wbuf.at[z * 2, kc], s0.at[kc])
        own_send(kc)

    @pl.when(xh == 1)
    def _():
        for kc in range(NCH):
            send(stage.at[kc], wbuf.at[z * 2, kc], s_swap, s0.at[kc], dev_x)

    @pl.when(xh == 0)
    def _():
        for kc in range(3):
            own_send(kc)

    with jax.named_scope("norm_rest"):
        lax.fori_loop(2, 8, norm_pair, 0)

    @pl.when(xh == 0)
    def _():
        own_send(3)
        own_send(4)

    @pl.when(xh == 1)
    def _():
        swapped_send(0)

    def hidden_step(n, carry):
        wait_for(w1.at[n], lsem.at[n])
        value = jnp.dot(mer[...], w1[n], preferred_element_type=F32)
        value = value + b1_ref[pl.ds(pl.multiple_of(n * CH, CH), CH)].reshape(1, CH)
        value = 0.5 * value * (1.0 + lax.erf(value * SQRT_HALF))
        hid[0, n] = value.astype(BF16)
        send(hid.at[0, n], hid.at[1, n], s_h, r_h1.at[n], dev_x)
        send(hid.at[0, n], hid.at[2, n], s_h, r_h2.at[n], dev_yb)

        @pl.when((xh == 1) & ((n == 1) | (n == 4)))
        def _():
            swapped_send(lax.div(n, 4) + 1)

        return carry

    loop("hidden_step", NCH, hidden_step)

    pltpu.make_async_copy(text_hbm, text, lsem.at[NCH + 1]).start()

    def far(kc):
        wait_for(wbuf.at[zm * 2, kc], r_om.at[kc])
        upper = wbuf.at[zm * 2, kc, pl.ds(0, CH // 2)]
        send(upper, upper, s_w, r_fm.at[kc], dev_zp)
        wait_for(wbuf.at[zp * 2, kc], r_op.at[kc])
        under = wbuf.at[zp * 2, kc, pl.ds(CH // 2, CH // 2)]
        send(under, under, s_w, r_fp.at[kc], dev_zm)
        if kc == 0:
            send(wbuf.at[zm * 2, 0], wbuf.at[zm * 2 + 1, 0], s_w, r_pm, dev_ya)
            send(wbuf.at[zp * 2, 0], wbuf.at[zp * 2 + 1, 0], s_w, r_pp, dev_ya)

    def late_own(kc):
        @pl.when(xh == 1)
        def _():
            swapped_send(kc)

    def pair(kc):
        block = wbuf.at[z * 2 + 1, kc]
        wait_for(block, r_p.at[kc])
        if kc > 0:
            send(block, block, s_w, r_pm, dev_zp)
            send(block, block, s_w, r_pp, dev_zm)

    def rows_x(n):
        wait_for(hid.at[1, n], r_h1.at[n])
        for half in range(2):

            @pl.when(xh == half)
            def _():
                top = pl.ds(0, HEADS[half])
                send(hid.at[1, n, top], hid.at[3, n, top], s_h, r_h3, dev_yb)

    def rows_y(n):
        wait_for(hid.at[2, n], r_h2.at[n])
        for half in range(2):

            @pl.when(xh == half)
            def _():
                rest = pl.ds(HEADS[half], CH - HEADS[half])
                send(hid.at[2, n, rest], hid.at[3, n, rest], s_h, r_h3, dev_x)

    def across_y(n):
        wait_for(wbuf.at[zo * 2, n, pl.ds(0, CH // 2)], r_fm.at[n])
        wait_for(wbuf.at[zo * 2, n, pl.ds(CH // 2, CH // 2)], r_fp.at[n])
        send(wbuf.at[zo * 2, n], wbuf.at[zo * 2 + 1, n], s_w, r_p2, dev_ya)

    def tile(rows, group, p):
        count = len(rows) * CH
        left = jnp.concatenate(
            [hid[rows[0] : rows[-1] + 1, n].reshape(count, CH) for n in range(NCH)],
            axis=1,
        )
        right = wbuf[group * 2 + p].reshape(NCH * CH, CH)
        return jnp.dot(left, right, preferred_element_type=F32)

    swap = lax.rem(z + c, 2)

    def pick(a, b, first):
        return a * first + b * (1 - first)

    def column_of(p):
        return (y + p * (3 - 2 * y)) * 2 + q

    def tiles(same, opposite):
        if same is None or opposite is None:
            to_z, to_p = my_z, my_p = opposite if same is None else same
        else:
            to_z = pick(same[0], opposite[0], swap)
            to_p = pick(same[1], opposite[1], swap)
            my_z = pick(opposite[0], same[0], swap)
            my_p = pick(opposite[1], same[1], swap)
        to_half = lax.rem(lax.div(to_z, 2) + xh + 1, 2)
        my_half = lax.rem(lax.div(my_z, 2) + xh + 1, 2)

        def give(rows):
            value = tile(rows, to_z, to_p).astype(BF16)

            def out():
                for i, r in enumerate(rows):
                    dsend[to_half, to_p, r] = value[i * CH : (i + 1) * CH]
                    send(
                        dsend.at[to_half, to_p, r],
                        drecv.at[to_half, to_p, r],
                        s_d,
                        r_d.at[to_half * 8 + to_p * 4 + r],
                        dev_core,
                    )

            return out

        def take(rows):
            value = tile(rows, my_z, my_p)

            def out():
                for i, r in enumerate(rows):
                    wait_for(
                        drecv.at[my_half, my_p, r], r_d.at[my_half * 8 + my_p * 4 + r]
                    )
                    mine = value[i * CH : (i + 1) * CH]
                    mine = mine + drecv[my_half, my_p, r].astype(F32)

                    @pl.when(my_half == 0)
                    def _():
                        xsend[my_p, r] = mine.astype(BF16)
                        there = r + 1 - 2 * (r % 2)
                        send(
                            xsend.at[my_p, r],
                            xrecv.at[my_p, there],
                            s_x,
                            r_x.at[my_p * 4 + there],
                            dev_cut,
                        )

                    @pl.when(my_half == 1)
                    def _():
                        column = pl.multiple_of(column_of(my_p) * CH, CH)
                        fbuf[my_p, r] = mine + b2_ref[:, pl.ds(column, CH)]

            return out

        return give, take

    near_a = tiles((z, 0), (zm, 0))
    near_b = tiles((z, 1), (zp, 0))
    middle = tiles((zo, 0), None)
    far_a = tiles((zo, 1), (zm, 1))
    far_b = tiles(None, (zp, 1))

    def give_near(r):
        with jax.named_scope(f"give_near{r}"):
            outs = [near_a[0]([r]), near_b[0]([r])]
            for out in outs:
                out()

    def take_near(r):
        with jax.named_scope(f"take_near{r}"):
            outs = [near_a[1]([r]), near_b[1]([r])]
            for out in outs:
                out()

    def run_single(name, steps, mine, rows):
        with jax.named_scope(name):

            @pl.when(swap != mine)
            def _():
                steps[0](rows)()

            @pl.when(swap == mine)
            def _():
                steps[1](rows)()

    def text_step(i, carry):
        rows = pl.ds(pl.multiple_of(i * CH, CH), CH)
        total = jnp.zeros((CH, CH), F32)
        for j in range(8):
            values = text[rows, j * CH : (j + 1) * CH].astype(F32)
            total = total + values * values
        sbuf[t, :, rows] = row_squares(total)
        return carry

    def step(label, work, *args):
        with jax.named_scope(label):
            work(*args)

    step("rows_y0", rows_y, 0)
    late_own(3)
    step("rows_y1", rows_y, 1)
    late_own(4)
    step("far0", far, 0)
    step("far1", far, 1)
    with jax.named_scope("text_in"):
        wait_for(text, lsem.at[NCH + 1])
    loop("text_step", 2, text_step)
    step("far2", far, 2)
    step("rows_y2", rows_y, 2)
    step("rows_x0", rows_x, 0)
    step("far3", far, 3)
    step("rows_y3", rows_y, 3)
    step("far4", far, 4)
    step("pair01", pair, 0)
    pair(1)
    step("rows_x1", rows_x, 1)
    step("rows_y4", rows_y, 4)
    pair(2)
    pair(3)
    pair(4)
    give_near(0)
    step("across_y0", across_y, 0)
    step("rows_x2", rows_x, 2)
    give_near(2)
    step("across_y1", across_y, 1)
    take_near(0)
    step("rows_x3", rows_x, 3)
    step("across_y2", across_y, 2)
    take_near(2)
    step("across_y3", across_y, 3)
    step("rows_x4", rows_x, 4)
    give_near(1)
    step("across_y4", across_y, 4)
    run_single("middle", middle, 0, [0, 1, 2])
    take_near(1)
    with jax.named_scope("diagonal"):
        wait_for(hid.at[3], r_h3)
    give_near(3)
    run_single("middle3", middle, 0, [3])
    take_near(3)

    def target(r, k):
        row_y = y + lax.div(r, 2) * (yb - y)
        row_x = xl + lax.rem(r, 2) * (1 - 2 * xl)
        return lax.rem(z * 8 + row_y * 2 + row_x + k, SHARDS)

    def pieces(p, r, k):
        rows = pl.ds(k * CAP, CAP)
        return obuf.at[p, r, rows], img.at[column_of(p), rows]

    def finish(p, r):
        with jax.named_scope(f"finish{p}{r}"):
            wait_for(xrecv.at[p, r], r_x.at[p * 4 + r])
            obuf[p, r] = (fbuf[p, r] + xrecv[p, r].astype(F32)).astype(BF16)
            for k in range(4):
                e = target(r, k)
                src, dst = pieces(p, r, k)

                @pl.when(e == d)
                def _():
                    pltpu.make_async_copy(src, dst, r_i).start()

                @pl.when(e != d)
                def _():
                    send(src, dst, s_i.at[p * 16 + r * 4 + k], r_i, (e, t))

    def finish_early(r):
        @pl.when(t != zo)
        def _():
            finish(0, r)

    finish_early(1)
    with jax.named_scope("pair_blocks"):
        wait_for(wbuf.at[zo * 2 + 1], r_p2)
        wait_for(wbuf.at[zm * 2 + 1], r_pm)
    every = [0, 1, 2, 3]
    with jax.named_scope("give_far"):
        far_a[0](every)()
    finish_early(3)
    with jax.named_scope("take_far"):
        far_a[1](every)()
    with jax.named_scope("pair_blocks"):
        wait_for(wbuf.at[zp * 2 + 1], r_pp)
    run_single("far_b", far_b, 1, every)
    finish_early(0)

    @pl.when(t == zo)
    def _():
        for r in (1, 3, 0):
            finish(0, r)

    finish(0, 2)
    for r in (1, 0, 3, 2):
        finish(1, r)

    with jax.named_scope("image_in"):
        wait_for(img, r_i)
    img_copy = pltpu.make_async_copy(img, img_out, lsem.at[0])
    img_copy.start()
    total = jnp.zeros((CH, CH), F32)
    for b in range(8):
        values = img[b].astype(F32)
        total = total + values * values
    sbuf[t, :, pl.ds(512, CH)] = row_squares(total)
    for i in range(1, 4):
        send(
            sbuf.at[t],
            sbuf.at[t],
            s_s.at[i - 1],
            r_s.at[i - 1],
            (d, lax.rem(t + i, 4)),
        )
    with jax.named_scope("sums_in"):
        for i in range(1, 4):
            wait_for(sbuf.at[lax.rem(t + 4 - i, 4)], r_s.at[i - 1])
    sums_copy = pltpu.make_async_copy(sbuf, sums_out, lsem.at[1])
    sums_copy.start()

    wait_for(wbuf.at[pl.ds(0, 7)], s_w)

    @pl.when(xh == 1)
    def _():
        wait_for(wbuf.at[0], s_swap)

    wait_for(hid.at[pl.ds(0, 3)], s_h)
    wait_for(dsend, s_d)
    wait_for(xsend, s_x)
    for p in range(2):

        def drain(r, carry):
            for k in range(4):
                src, _unused = pieces(p, r, k)

                @pl.when(target(r, k) != d)
                def _():
                    wait_for(src, s_i.at[p * 16 + r * 4 + k])

            return carry

        loop("drain", 4, drain)
    for i in range(1, 4):
        wait_for(sbuf.at[t], s_s.at[i - 1])
    img_copy.wait()
    sums_copy.wait()


def splice_kernel(
    grids_ref, routing_ref, text_ref, img_ref, sums_ref, gain_ref, emb_ref, out_ref
):
    d = lax.axis_index("dp")
    g = pl.program_id(0)
    rows = text_ref.shape[0]
    starts = []
    total = jnp.int32(0)
    for k in range(4):
        s = lax.rem(d + SHARDS - k, SHARDS)
        count = jnp.int32(0)
        for b in range(4):
            size = grids_ref[b, 0, s] * grids_ref[b, 1, s]
            count = count + jnp.where(routing_ref[b, s] == k, size, 0)
        starts.append(total)
        total = total + count
    position = g * rows + lax.broadcasted_iota(jnp.int32, (rows, 1), 0)
    source = position
    for k in range(1, 4):
        begin = jnp.where(position >= starts[k], k * CAP - starts[k], 0)
        if k > 1:
            begin = begin - jnp.where(
                position >= starts[k], (k - 1) * CAP - starts[k - 1], 0
            )
        source = source + begin
    live = position < total
    sums = sums_ref[0] + sums_ref[1] + sums_ref[2] + sums_ref[3]
    sums = sums[0:1, :]
    index = jnp.where(live, 512 + source, position)
    lanes = lax.broadcasted_iota(jnp.int32, (rows, sums.shape[1]), 1)
    square = jnp.sum(jnp.where(lanes == index, sums, 0.0), axis=-1, keepdims=True)
    scale = lax.rsqrt(square / D + 1e-06)
    picks = jnp.where(
        lax.broadcasted_iota(jnp.int32, (rows, 4 * CAP), 1) == source, 1.0, 0.0
    ).astype(BF16)
    blocks = img_ref.shape[0]

    @pl.when(g * rows < 4 * CAP)
    def _():
        for b in range(blocks):
            cols = slice(b * CH, (b + 1) * CH)
            taken = jnp.dot(picks, img_ref[b], preferred_element_type=F32)
            value = jnp.where(live, taken, text_ref[:, cols].astype(F32))
            emb_ref[:, cols] = value.astype(BF16)
            out_ref[:, cols] = (value * scale * gain_ref[:, cols]).astype(BF16)

    @pl.when(g * rows >= 4 * CAP)
    def _():
        for b in range(blocks):
            cols = slice(b * CH, (b + 1) * CH)
            value = text_ref[:, cols].astype(F32)
            emb_ref[:, cols] = text_ref[:, cols]
            out_ref[:, cols] = (value * scale * gain_ref[:, cols]).astype(BF16)


def per_device(
    patches,
    norm_gain,
    norm_bias,
    first_weight,
    first_bias,
    second_weight,
    second_bias,
    text_embeds,
    final_gain,
    image_grids,
    routing,
):
    seq, features = text_embeds.shape
    width = patches.shape[1]
    hbm = pl.BlockSpec(memory_space=pl.ANY)
    vmem = pl.BlockSpec(memory_space=pltpu.VMEM)
    smem = pl.BlockSpec(memory_space=pltpu.SMEM)
    dma = pltpu.SemaphoreType.DMA
    img, sums = pl.pallas_call(
        merge_kernel,
        out_shape=(
            jax.ShapeDtypeStruct((8, CH, CH), BF16),
            jax.ShapeDtypeStruct((4, 8, seq + CH), F32),
        ),
        in_specs=[smem, hbm, vmem, vmem, hbm, vmem, hbm, vmem, hbm],
        out_specs=(hbm, hbm),
        scratch_shapes=[
            pltpu.VMEM(patches.shape, BF16),
            pltpu.VMEM((NCH, first_weight.shape[0], CH), BF16),
            pltpu.VMEM((2, width // 128, 64, 128), F32),
            pltpu.VMEM((CH, 4 * width), BF16),
            pltpu.VMEM((4, NCH, CH, CH), BF16),
            pltpu.VMEM((8, NCH, CH, CH), BF16),
            pltpu.VMEM((NCH, CH, CH), BF16),
            pltpu.VMEM((seq, features), BF16),
            pltpu.VMEM((2, 2, 4, CH, CH), BF16),
            pltpu.VMEM((2, 2, 4, CH, CH), BF16),
            pltpu.VMEM((2, 4, CH, CH), BF16),
            pltpu.VMEM((2, 4, CH, CH), BF16),
            pltpu.VMEM((2, 4, CH, CH), F32),
            pltpu.VMEM((2, 4, CH, CH), BF16),
            pltpu.VMEM((8, CH, CH), BF16),
            pltpu.VMEM((4, 8, seq + CH), F32),
            dma((NCH + 2,)),
            dma((NCH,)),
            dma,
            dma,
            dma,
            dma,
            dma,
            dma,
            dma((32,)),
            dma((3,)),
            dma((NCH,)),
            dma((NCH,)),
            dma((NCH,)),
            dma((NCH,)),
            dma((NCH,)),
            dma,
            dma,
            dma,
            dma((NCH,)),
            dma((NCH,)),
            dma,
            dma((16,)),
            dma((8,)),
            dma,
            dma((3,)),
        ],
        compiler_params=pltpu.CompilerParams(
            collective_id=0, has_side_effects=True, vmem_limit_bytes=60 * 1024 * 1024
        ),
        name="merge",
    )(
        routing.T,
        patches,
        norm_gain,
        norm_bias,
        first_weight,
        first_bias,
        second_weight.reshape(NCH, CH, CH),
        second_bias.reshape(1, -1),
        text_embeds,
    )
    rows = 128
    return pl.pallas_call(
        splice_kernel,
        grid=(seq // rows,),
        out_shape=(
            jax.ShapeDtypeStruct((seq, features), BF16),
            jax.ShapeDtypeStruct((seq, features), BF16),
        ),
        in_specs=[
            smem,
            smem,
            pl.BlockSpec((rows, features), lambda g: (g, 0)),
            vmem,
            vmem,
            vmem,
        ],
        out_specs=(
            pl.BlockSpec((rows, features), lambda g: (g, 0)),
            pl.BlockSpec((rows, features), lambda g: (g, 0)),
        ),
        name="splice",
    )(
        image_grids.transpose(1, 2, 0),
        routing.T,
        text_embeds,
        img,
        sums,
        final_gain.reshape(1, -1),
    )


def solution(mesh):
    placed = (
        P("dp", None),
        P(),
        P(),
        P(None, "tensor"),
        P("tensor"),
        P("tensor", "dp"),
        P("tensor"),
        P("dp", "tensor"),
        P("tensor"),
        P(),
        P(),
    )
    return jax.shard_map(
        per_device,
        mesh=mesh,
        in_specs=placed,
        out_specs=(P("dp", "tensor"), P("dp", "tensor")),
        check_vma=False,
    )
```

```python
import functools

import jax
import jax.numpy as jnp
from jax import lax
from jax.experimental import pallas as pl
from jax.experimental.pallas import tpu as pltpu
from jax.sharding import PartitionSpec as P

MESH = pl.DeviceIdType.MESH
F32 = jnp.float32
BF16 = jnp.bfloat16
SHARDS = 32
CAP = 64
D = 8192
CH = 256
NCH = 5
HEADS = (128, 208)
SQRT_HALF = 0.7071067811865476


def wait_for(ref, sem):
    pltpu.make_async_copy(ref, ref, sem).wait()


def send(src, dst, send_sem, recv_sem, device):
    pltpu.make_async_remote_copy(
        src_ref=src,
        dst_ref=dst,
        send_sem=send_sem,
        recv_sem=recv_sem,
        device_id=device,
        device_id_type=MESH,
    ).start()


def loop(name, count, step):
    with jax.named_scope(name):
        lax.fori_loop(0, count, step, 0)


def row_squares(values):
    ones = jnp.ones((8, values.shape[1]), F32)
    return lax.dot_general(
        ones,
        values,
        (((1,), (1,)), ((), ())),
        precision=lax.Precision.HIGHEST,
        preferred_element_type=F32,
    )


def merge_kernel(
    routing_hbm,
    pat_hbm,
    gain_hbm,
    nbias_hbm,
    w1_hbm,
    b1_hbm,
    w2_hbm,
    b2_hbm,
    text_hbm,
    img_out,
    tsums_out,
    isums_out,
    routing_ref,
    gain_ref,
    nbias_ref,
    b1_ref,
    b2_ref,
    pat,
    w1,
    nbuf,
    mer,
    hid,
    wbuf,
    stage,
    text,
    dsend,
    drecv,
    xsend,
    xrecv,
    fbuf,
    obuf,
    img,
    tbuf,
    ibuf,
    lsem,
    s_small,
    s0,
    s_first,
    s_stage,
    s_swap,
    s_w,
    s_h,
    s_d,
    s_x,
    s_i,
    s_t,
    s_s,
    r_om,
    r_op,
    r_p,
    r_fm,
    r_fp,
    r_pm,
    r_pp,
    r_p2,
    r_h1,
    r_h2,
    r_h3,
    r_d,
    r_x,
    r_i,
    r_t,
    r_s,
):
    d = lax.axis_index("dp")
    t = lax.axis_index("tensor")
    z = lax.div(d, 8)
    y = lax.rem(lax.div(d, 2), 4)
    xl = lax.rem(d, 2)
    xh = lax.div(t, 2)
    c = lax.rem(t, 2)
    zp = lax.rem(z + 1, 4)
    zm = lax.rem(z + 3, 4)
    zo = lax.rem(z + 2, 4)
    yb = y + 1 - 2 * lax.rem(y, 2)
    q = xl + xh - 2 * xl * xh
    dev_zp = (zp * 8 + y * 2 + xl, t)
    dev_zm = (zm * 8 + y * 2 + xl, t)
    dev_ya = (z * 8 + (3 - y) * 2 + xl, t)
    dev_yb = (z * 8 + yb * 2 + xl, t)
    dev_x = (z * 8 + y * 2 + 1 - xl, t)
    dev_cut = (z * 8 + y * 2 + 1 - xl, (1 - xh) * 2 + c)
    dev_core = (d, xh * 2 + 1 - c)

    @pl.when(xh == 0)
    def _():
        pltpu.make_async_copy(w2_hbm, wbuf.at[z * 2], s_stage).start()

    @pl.when(xh == 1)
    def _():
        pltpu.make_async_copy(w2_hbm, stage, s_stage).start()

    pltpu.make_async_copy(pat_hbm, pat, lsem.at[NCH]).start()

    small = [
        pltpu.make_async_copy(src, dst, s_small.at[i])
        for i, (src, dst) in enumerate(
            (
                (routing_hbm, routing_ref),
                (gain_hbm, gain_ref),
                (nbias_hbm, nbias_ref),
                (b1_hbm, b1_ref),
                (b2_hbm, b2_ref),
            )
        )
    ]
    for copy in small:
        copy.start()

    barrier = pltpu.get_barrier_semaphore()
    base = d - lax.rem(d, 4)

    def greet(device):
        pl.semaphore_signal(barrier, inc=1, device_id=device, device_id_type=MESH)

    for o in range(-4, 8):
        other = lax.rem(base + o + SHARDS, SHARDS)

        @pl.when(other != d)
        def _():
            greet((other, t))

    greet(dev_zp)
    greet(dev_zm)
    greet(dev_cut)
    for i in range(1, 4):
        greet((d, lax.rem(t + i, 4)))

    for copy in small:
        copy.wait()

    width = pat.shape[1]
    gain = gain_ref[...].reshape(1, width)
    nbias = nbias_ref[...].reshape(1, width)

    def norm_pair(pair, carry):
        for u in range(2):
            norm_step(pair * 2 + u, nbuf.at[u])
        return carry

    def norm_step(step, nbuf):
        slot = lax.div(step, 4)
        part = lax.rem(step, 4)
        values = jnp.zeros((64, width), BF16)
        for b in range(4):
            start = pl.multiple_of(b * (4 * CAP) + part * 64, 64)
            chosen = (routing_ref[b, d] == slot).astype(F32).astype(BF16)
            values = values + pat[pl.ds(start, 64), :] * chosen
        values = values.astype(F32)
        centered = values - jnp.mean(values, axis=-1, keepdims=True)
        variance = jnp.mean(centered * centered, axis=-1, keepdims=True)
        normed = centered * lax.rsqrt(variance + 1e-06) * gain + nbias
        row = pl.multiple_of(step * 16, 16)
        for i in range(width // 128):
            nbuf[i] = normed[:, i * 128 : (i + 1) * 128]
        for j in range(4):
            for i in range(width // 128):
                mer[pl.ds(row, 16), j * width + i * 128 : j * width + (i + 1) * 128] = (
                    nbuf[i, pl.ds(j, 16, stride=4), :].astype(BF16)
                )

    with jax.named_scope("patches_in"):
        wait_for(pat, lsem.at[NCH])
    for n in range(NCH):
        pltpu.make_async_copy(
            w1_hbm.at[:, pl.ds(n * CH, CH)], w1.at[n], lsem.at[n]
        ).start()
    with jax.named_scope("norm_first"):
        lax.fori_loop(0, 2, norm_pair, 0)
    with jax.named_scope("greeting"):
        pl.semaphore_wait(barrier, 17)

    def own_send(kc, part=pl.ds(0, CH)):
        block = wbuf.at[z * 2, kc, part]
        send(block, block, s_w, r_om.at[kc], dev_zp)
        send(block, block, s_w, r_op.at[kc], dev_zm)
        send(block, wbuf.at[z * 2 + 1, kc, part], s_w, r_p.at[kc], dev_ya)

    with jax.named_scope("second_in"):
        wait_for(stage, s_stage)

    halves = (pl.ds(0, CH // 2), pl.ds(CH // 2, CH // 2))

    def swapped_half(half):
        with jax.named_scope("swapped"):
            wait_for(wbuf.at[z * 2, 0, halves[half]], s_first.at[half])
        own_send(0, halves[half])

    def swapped_send(kc):
        with jax.named_scope("swapped"):
            wait_for(wbuf.at[z * 2, kc], s0.at[kc])
        own_send(kc)

    @pl.when(xh == 1)
    def _():
        for half in range(2):
            send(
                stage.at[0, halves[half]],
                wbuf.at[z * 2, 0, halves[half]],
                s_swap,
                s_first.at[half],
                dev_x,
            )
        for kc in range(1, NCH):
            send(stage.at[kc], wbuf.at[z * 2, kc], s_swap, s0.at[kc], dev_x)

    @pl.when(xh == 0)
    def _():
        for kc in range(3):
            own_send(kc)

    with jax.named_scope("norm_rest"):
        lax.fori_loop(2, 8, norm_pair, 0)

    @pl.when(xh == 0)
    def _():
        own_send(3)
        own_send(4)

    @pl.when(xh == 1)
    def _():
        swapped_half(0)

    def hidden_step(n, carry):
        wait_for(w1.at[n], lsem.at[n])
        value = jnp.dot(mer[...], w1[n], preferred_element_type=F32)
        value = value + b1_ref[pl.ds(pl.multiple_of(n * CH, CH), CH)].reshape(1, CH)
        value = 0.5 * value * (1.0 + lax.erf(value * SQRT_HALF))
        hid[0, n] = value.astype(BF16)
        send(hid.at[0, n], hid.at[1, n], s_h, r_h1.at[n], dev_x)
        send(hid.at[0, n], hid.at[2, n], s_h, r_h2.at[n], dev_yb)

        @pl.when((xh == 1) & (n == 0))
        def _():
            swapped_half(1)

        @pl.when((xh == 1) & ((n == 2) | (n == 4)))
        def _():
            swapped_send(lax.div(n, 2))

        return carry

    loop("hidden_step", NCH, hidden_step)

    pltpu.make_async_copy(text_hbm, text, lsem.at[NCH + 1]).start()

    def far(kc):
        wait_for(wbuf.at[zm * 2, kc], r_om.at[kc])
        upper = wbuf.at[zm * 2, kc, pl.ds(0, CH // 2)]
        send(upper, upper, s_w, r_fm.at[kc], dev_zp)
        wait_for(wbuf.at[zp * 2, kc], r_op.at[kc])
        under = wbuf.at[zp * 2, kc, pl.ds(CH // 2, CH // 2)]
        send(under, under, s_w, r_fp.at[kc], dev_zm)
        if kc == 0:
            send(wbuf.at[zm * 2, 0], wbuf.at[zm * 2 + 1, 0], s_w, r_pm, dev_ya)
            send(wbuf.at[zp * 2, 0], wbuf.at[zp * 2 + 1, 0], s_w, r_pp, dev_ya)

    def late_own(kc):
        @pl.when(xh == 1)
        def _():
            swapped_send(kc)

    def pair(kc):
        block = wbuf.at[z * 2 + 1, kc]
        wait_for(block, r_p.at[kc])
        if kc > 0:
            send(block, block, s_w, r_pm, dev_zp)
            send(block, block, s_w, r_pp, dev_zm)

    def rows_x(n):
        wait_for(hid.at[1, n], r_h1.at[n])
        for half in range(2):

            @pl.when(xh == half)
            def _():
                top = pl.ds(0, HEADS[half])
                send(hid.at[1, n, top], hid.at[3, n, top], s_h, r_h3, dev_yb)

    def rows_y(n):
        wait_for(hid.at[2, n], r_h2.at[n])
        for half in range(2):

            @pl.when(xh == half)
            def _():
                rest = pl.ds(HEADS[half], CH - HEADS[half])
                send(hid.at[2, n, rest], hid.at[3, n, rest], s_h, r_h3, dev_x)

    def across_y(n):
        wait_for(wbuf.at[zo * 2, n, pl.ds(0, CH // 2)], r_fm.at[n])
        wait_for(wbuf.at[zo * 2, n, pl.ds(CH // 2, CH // 2)], r_fp.at[n])
        send(wbuf.at[zo * 2, n], wbuf.at[zo * 2 + 1, n], s_w, r_p2, dev_ya)

    def tile(rows, group, p):
        count = len(rows) * CH
        left = jnp.concatenate(
            [hid[rows[0] : rows[-1] + 1, n].reshape(count, CH) for n in range(NCH)],
            axis=1,
        )
        right = wbuf[group * 2 + p].reshape(NCH * CH, CH)
        return jnp.dot(left, right, preferred_element_type=F32)

    swap = lax.rem(z + c, 2)

    def pick(a, b, first):
        return a * first + b * (1 - first)

    def column_of(p):
        return (y + p * (3 - 2 * y)) * 2 + q

    def tiles(same, opposite):
        if same is None or opposite is None:
            to_z, to_p = my_z, my_p = opposite if same is None else same
        else:
            to_z = pick(same[0], opposite[0], swap)
            to_p = pick(same[1], opposite[1], swap)
            my_z = pick(opposite[0], same[0], swap)
            my_p = pick(opposite[1], same[1], swap)
        to_half = lax.rem(lax.div(to_z, 2) + xh + 1, 2)
        my_half = lax.rem(lax.div(my_z, 2) + xh + 1, 2)

        def give(rows):
            value = tile(rows, to_z, to_p).astype(BF16)

            def out():
                for i, r in enumerate(rows):
                    dsend[to_half, to_p, r] = value[i * CH : (i + 1) * CH]
                    send(
                        dsend.at[to_half, to_p, r],
                        drecv.at[to_half, to_p, r],
                        s_d,
                        r_d.at[to_half * 8 + to_p * 4 + r],
                        dev_core,
                    )

            return out

        def take(rows):
            value = tile(rows, my_z, my_p)

            def out():
                for i, r in enumerate(rows):
                    wait_for(
                        drecv.at[my_half, my_p, r], r_d.at[my_half * 8 + my_p * 4 + r]
                    )
                    mine = value[i * CH : (i + 1) * CH]
                    mine = mine + drecv[my_half, my_p, r].astype(F32)

                    @pl.when(my_half == 0)
                    def _():
                        xsend[my_p, r] = mine.astype(BF16)
                        there = r + 1 - 2 * (r % 2)
                        send(
                            xsend.at[my_p, r],
                            xrecv.at[my_p, there],
                            s_x,
                            r_x.at[my_p * 4 + there],
                            dev_cut,
                        )

                    @pl.when(my_half == 1)
                    def _():
                        column = pl.multiple_of(column_of(my_p) * CH, CH)
                        fbuf[my_p, r] = mine + b2_ref[:, pl.ds(column, CH)]

            return out

        return give, take

    near_a = tiles((z, 0), (zm, 0))
    near_b = tiles((z, 1), (zp, 0))
    middle = tiles((zo, 0), None)
    up = lax.rem(lax.div(zp, 2) + xh, 2)
    far_a = tiles((zo, 1), None)
    far_b = tiles(None, (pick(zp, zm, up), 1))
    far_c = tiles(None, (pick(zm, zp, up), 1))

    def give_near(r):
        with jax.named_scope(f"give_near{r}"):
            outs = [near_a[0]([r]), near_b[0]([r])]
            for out in outs:
                out()

    def take_near(r):
        with jax.named_scope(f"take_near{r}"):
            outs = [near_a[1]([r]), near_b[1]([r])]
            for out in outs:
                out()

    def run_single(name, steps, mine, rows):
        with jax.named_scope(name):

            @pl.when(swap != mine)
            def _():
                steps[0](rows)()

            @pl.when(swap == mine)
            def _():
                steps[1](rows)()

    def text_step(i, carry):
        rows = pl.ds(pl.multiple_of(i * CH, CH), CH)
        total = jnp.zeros((CH, CH), F32)
        for j in range(8):
            values = text[rows, j * CH : (j + 1) * CH].astype(F32)
            total = total + values * values
        tbuf[t, :, rows] = row_squares(total)
        return carry

    def share(buf, send_sems, recv_sems):
        for i in range(1, 4):
            send(
                buf.at[t],
                buf.at[t],
                send_sems.at[i - 1],
                recv_sems.at[i - 1],
                (d, lax.rem(t + i, 4)),
            )

    def step(label, work, *args):
        with jax.named_scope(label):
            work(*args)

    step("rows_y0", rows_y, 0)
    late_own(3)
    step("rows_y1", rows_y, 1)
    late_own(4)
    step("far0", far, 0)
    step("far1", far, 1)
    with jax.named_scope("text_in"):
        wait_for(text, lsem.at[NCH + 1])
    loop("text_step", 2, text_step)
    share(tbuf, s_t, r_t)
    step("far2", far, 2)
    step("rows_y2", rows_y, 2)
    step("rows_x0", rows_x, 0)
    step("far3", far, 3)
    step("rows_y3", rows_y, 3)
    step("far4", far, 4)
    step("pair01", pair, 0)
    pair(1)
    step("rows_x1", rows_x, 1)
    step("rows_y4", rows_y, 4)
    pair(2)
    pair(3)
    pair(4)
    give_near(0)
    step("across_y0", across_y, 0)
    step("rows_x2", rows_x, 2)
    give_near(2)
    step("across_y1", across_y, 1)
    take_near(0)
    step("rows_x3", rows_x, 3)
    step("across_y2", across_y, 2)
    take_near(2)
    step("across_y3", across_y, 3)
    step("rows_x4", rows_x, 4)
    give_near(1)
    step("across_y4", across_y, 4)
    run_single("middle", middle, 0, [0, 1, 2])
    take_near(1)
    with jax.named_scope("diagonal"):
        wait_for(hid.at[3], r_h3)
    give_near(3)
    run_single("middle3", middle, 0, [3])
    take_near(3)

    def target(r, k):
        row_y = y + lax.div(r, 2) * (yb - y)
        row_x = xl + lax.rem(r, 2) * (1 - 2 * xl)
        return lax.rem(z * 8 + row_y * 2 + row_x + k, SHARDS)

    def pieces(p, r, k):
        rows = pl.ds(k * CAP, CAP)
        return obuf.at[p, r, rows], img.at[column_of(p), rows]

    def finish(p, r):
        with jax.named_scope(f"finish{p}{r}"):
            wait_for(xrecv.at[p, r], r_x.at[p * 4 + r])
            obuf[p, r] = (fbuf[p, r] + xrecv[p, r].astype(F32)).astype(BF16)
            for k in range(4):
                e = target(r, k)
                src, dst = pieces(p, r, k)

                @pl.when(e == d)
                def _():
                    pltpu.make_async_copy(src, dst, r_i).start()

                @pl.when((e != d) & (lax.div(e, 4) == lax.div(d, 4)))
                def _():
                    send(src, dst, s_i.at[p * 16 + r * 4 + k], r_i, (e, t))

    def onward(p, r):
        for k in range(1, 4):
            e = target(r, k)
            src, dst = pieces(p, r, k)

            @pl.when(lax.div(e, 4) != lax.div(d, 4))
            def _():
                send(src, dst, s_i.at[p * 16 + r * 4 + k], r_i, (e, t))

    def on_side(side, *work):
        @pl.when(xh == side)
        def _():
            for do, p, rows in work:
                for r in rows:
                    do(p, r)

    @pl.when((xh == 0) & (t != zo))
    def _():
        finish(0, 1)

    on_side(1, (finish, 0, (1, 3, 0, 2)))
    every = [0, 1, 2, 3]
    with jax.named_scope("pair_blocks_o"):
        wait_for(wbuf.at[zo * 2 + 1], r_p2)
    run_single("far_a", far_a, 0, every)

    @pl.when((xh == 0) & (t == zo))
    def _():
        finish(0, 1)

    on_side(0, (onward, 0, (1,)), (finish, 0, (3,)), (onward, 0, (3,)))
    on_side(1, (onward, 0, (1, 3, 0, 2)))
    with jax.named_scope("pair_blocks"):
        wait_for(wbuf.at[zm * 2 + 1], r_pm)
        wait_for(wbuf.at[zp * 2 + 1], r_pp)
    run_single("far_b", far_b, 1, every)
    on_side(0, (finish, 0, (0,)), (onward, 0, (0,)))
    run_single("far_c", far_c, 1, every)
    on_side(0, (finish, 0, (2,)), (onward, 0, (2,)))
    for r in (1, 0, 3, 2):
        finish(1, r)
        onward(1, r)

    with jax.named_scope("image_in"):
        wait_for(img, r_i)
    img_copy = pltpu.make_async_copy(img, img_out, lsem.at[0])
    img_copy.start()
    total = jnp.zeros((CH, CH), F32)
    for b in range(8):
        values = img[b].astype(F32)
        total = total + values * values
    ibuf[t] = row_squares(total)
    share(ibuf, s_s, r_s)
    for i in range(1, 4):
        wait_for(tbuf.at[lax.rem(t + 4 - i, 4)], r_t.at[i - 1])
    text_copy = pltpu.make_async_copy(tbuf, tsums_out, lsem.at[2])
    text_copy.start()
    with jax.named_scope("sums_in"):
        for i in range(1, 4):
            wait_for(ibuf.at[lax.rem(t + 4 - i, 4)], r_s.at[i - 1])
    sums_copy = pltpu.make_async_copy(ibuf, isums_out, lsem.at[1])
    sums_copy.start()

    wait_for(wbuf.at[pl.ds(0, 7)], s_w)

    @pl.when(xh == 1)
    def _():
        wait_for(wbuf.at[0], s_swap)

    wait_for(hid.at[pl.ds(0, 3)], s_h)
    wait_for(dsend, s_d)
    wait_for(xsend, s_x)
    for p in range(2):

        def drain(r, carry):
            for k in range(4):
                src, _unused = pieces(p, r, k)

                @pl.when(target(r, k) != d)
                def _():
                    wait_for(src, s_i.at[p * 16 + r * 4 + k])

            return carry

        loop("drain", 4, drain)
    for i in range(1, 4):
        wait_for(tbuf.at[t], s_t.at[i - 1])
        wait_for(ibuf.at[t], s_s.at[i - 1])
    img_copy.wait()
    text_copy.wait()
    sums_copy.wait()


def splice_kernel(
    grids_ref,
    routing_ref,
    text_hbm,
    img_hbm,
    tsums_hbm,
    isums_hbm,
    gain_hbm,
    emb_hbm,
    out_hbm,
    text,
    img,
    tsums,
    isums,
    gain,
    emb,
    out,
    in_sem,
    emb_sem,
    out_sem,
):
    rows = 128
    images = 4 * CAP
    steps = text.shape[0] // rows
    first = images // rows

    def part(ref, i):
        return ref.at[pl.ds(i * rows, rows)]

    small = [
        pltpu.make_async_copy(tsums_hbm, tsums, in_sem.at[steps]),
        pltpu.make_async_copy(isums_hbm, isums, in_sem.at[steps + 1]),
        pltpu.make_async_copy(gain_hbm, gain, in_sem.at[steps + 2]),
    ]
    whole = pltpu.make_async_copy(img_hbm, img, in_sem.at[steps + 3])
    order = list(range(first, steps)) + list(range(first))
    loads = {
        i: pltpu.make_async_copy(part(text_hbm, i), part(text, i), in_sem.at[i])
        for i in order
    }
    for copy in small[:1] + small[2:]:
        copy.start()
    for i in order[: steps - first]:
        loads[i].start()
    whole.start()
    small[1].start()
    for i in order[steps - first :]:
        loads[i].start()

    d = lax.axis_index("dp")
    starts = []
    total = jnp.int32(0)
    for k in range(4):
        s = lax.rem(d + SHARDS - k, SHARDS)
        count = jnp.int32(0)
        for b in range(4):
            size = grids_ref[b, 0, s] * grids_ref[b, 1, s]
            count = count + jnp.where(routing_ref[b, s] == k, size, 0)
        starts.append(total)
        total = total + count

    def picked(sums_ref, index):
        sums = sums_ref[0] + sums_ref[1] + sums_ref[2] + sums_ref[3]
        sums = sums[0:1, :]
        lanes = lax.broadcasted_iota(jnp.int32, (rows, sums.shape[1]), 1)
        return jnp.sum(jnp.where(lanes == index, sums, 0.0), axis=-1, keepdims=True)

    copies = []
    for copy in small[:1] + small[2:]:
        copy.wait()
    for i in order:
        position = i * rows + lax.broadcasted_iota(jnp.int32, (rows, 1), 0)
        square = picked(tsums, position)
        loads[i].wait()
        if i >= first:
            copies.append(
                pltpu.make_async_copy(part(text, i), part(emb_hbm, i), emb_sem.at[i])
            )
            copies[-1].start()
            scale = lax.rsqrt(square / D + 1e-06)
        else:
            if i == 0:
                whole.wait()
                small[1].wait()
            source = position
            for k in range(1, 4):
                shift = k * CAP - starts[k]
                if k > 1:
                    shift = shift - ((k - 1) * CAP - starts[k - 1])
                source = source + jnp.where(position >= starts[k], shift, 0)
            live = position < total
            square = jnp.where(live, picked(isums, source), square)
            scale = lax.rsqrt(square / D + 1e-06)
            picks = jnp.where(
                lax.broadcasted_iota(jnp.int32, (rows, images), 1) == source, 1.0, 0.0
            ).astype(BF16)
        here = slice(i * rows, (i + 1) * rows)
        for b in range(img.shape[0]):
            cols = slice(b * CH, (b + 1) * CH)
            value = text[here, cols].astype(F32)
            if i < first:
                taken = jnp.dot(picks, img[b], preferred_element_type=F32)
                value = jnp.where(live, taken, value)
                emb[here, cols] = value.astype(BF16)
            out[here, cols] = (value * scale * gain[:, cols]).astype(BF16)
        if i < first:
            copies.append(
                pltpu.make_async_copy(part(emb, i), part(emb_hbm, i), emb_sem.at[i])
            )
            copies[-1].start()
        copies.append(
            pltpu.make_async_copy(part(out, i), part(out_hbm, i), out_sem.at[i])
        )
        copies[-1].start()
    for copy in copies:
        copy.wait()


def per_device(
    patches,
    norm_gain,
    norm_bias,
    first_weight,
    first_bias,
    second_weight,
    second_bias,
    text_embeds,
    final_gain,
    image_grids,
    routing,
):
    seq, features = text_embeds.shape
    width = patches.shape[1]
    anywhere = pl.BlockSpec(memory_space=pl.ANY)
    smem = pl.BlockSpec(memory_space=pltpu.SMEM)
    dma = pltpu.SemaphoreType.DMA
    img, tsums, isums = pl.pallas_call(
        merge_kernel,
        out_shape=(
            jax.ShapeDtypeStruct((8, CH, CH), BF16),
            jax.ShapeDtypeStruct((4, 8, seq), F32),
            jax.ShapeDtypeStruct((4, 8, CH), F32),
        ),
        in_specs=[pl.BlockSpec(memory_space=pltpu.HBM)] * 9,
        out_specs=(anywhere, anywhere, anywhere),
        scratch_shapes=[
            pltpu.SMEM(routing.T.shape, jnp.int32),
            pltpu.VMEM(norm_gain.shape, F32),
            pltpu.VMEM(norm_bias.shape, F32),
            pltpu.VMEM(first_bias.shape, F32),
            pltpu.VMEM((1, second_bias.shape[0]), F32),
            pltpu.VMEM(patches.shape, BF16),
            pltpu.VMEM((NCH, first_weight.shape[0], CH), BF16),
            pltpu.VMEM((2, width // 128, 64, 128), F32),
            pltpu.VMEM((CH, 4 * width), BF16),
            pltpu.VMEM((4, NCH, CH, CH), BF16),
            pltpu.VMEM((8, NCH, CH, CH), BF16),
            pltpu.VMEM((NCH, CH, CH), BF16),
            pltpu.VMEM((seq, features), BF16),
            pltpu.VMEM((2, 2, 4, CH, CH), BF16),
            pltpu.VMEM((2, 2, 4, CH, CH), BF16),
            pltpu.VMEM((2, 4, CH, CH), BF16),
            pltpu.VMEM((2, 4, CH, CH), BF16),
            pltpu.VMEM((2, 4, CH, CH), F32),
            pltpu.VMEM((2, 4, CH, CH), BF16),
            pltpu.VMEM((8, CH, CH), BF16),
            pltpu.VMEM((4, 8, seq), F32),
            pltpu.VMEM((4, 8, CH), F32),
            dma((NCH + 2,)),
            dma((5,)),
            dma((NCH,)),
            dma((2,)),
            dma,
            dma,
            dma,
            dma,
            dma,
            dma,
            dma((32,)),
            dma((3,)),
            dma((3,)),
            dma((NCH,)),
            dma((NCH,)),
            dma((NCH,)),
            dma((NCH,)),
            dma((NCH,)),
            dma,
            dma,
            dma,
            dma((NCH,)),
            dma((NCH,)),
            dma,
            dma((16,)),
            dma((8,)),
            dma,
            dma((3,)),
            dma((3,)),
        ],
        compiler_params=pltpu.CompilerParams(
            collective_id=0, has_side_effects=True, vmem_limit_bytes=60 * 1024 * 1024
        ),
        name="merge",
    )(
        routing.T,
        patches,
        norm_gain,
        norm_bias,
        first_weight,
        first_bias,
        second_weight.reshape(NCH, CH, CH),
        second_bias.reshape(1, -1),
        text_embeds,
    )
    return pl.pallas_call(
        splice_kernel,
        out_shape=(
            jax.ShapeDtypeStruct((seq, features), BF16),
            jax.ShapeDtypeStruct((seq, features), BF16),
        ),
        in_specs=[smem, smem] + [anywhere] * 5,
        out_specs=(anywhere, anywhere),
        scratch_shapes=[
            pltpu.VMEM((seq, features), BF16),
            pltpu.VMEM(img.shape, BF16),
            pltpu.VMEM(tsums.shape, F32),
            pltpu.VMEM(isums.shape, F32),
            pltpu.VMEM((1, features), F32),
            pltpu.VMEM((4 * CAP, features), BF16),
            pltpu.VMEM((seq, features), BF16),
            dma((8,)),
            dma((4,)),
            dma((4,)),
        ],
        compiler_params=pltpu.CompilerParams(vmem_limit_bytes=60 * 1024 * 1024),
        name="splice",
    )(
        image_grids.transpose(1, 2, 0),
        routing.T,
        text_embeds,
        img,
        tsums,
        isums,
        final_gain.reshape(1, -1),
    )


def solution(mesh):
    placed = (
        P("dp", None),
        P(),
        P(),
        P(None, "tensor"),
        P("tensor"),
        P("tensor", "dp"),
        P("tensor"),
        P("dp", "tensor"),
        P("tensor"),
        P(),
        P(),
    )
    return jax.shard_map(
        per_device,
        mesh=mesh,
        in_specs=placed,
        out_specs=(P("dp", "tensor"), P("dp", "tensor")),
        check_vma=False,
    )
```

```python
import functools

import jax
import jax.numpy as jnp
from jax import lax
from jax.experimental import pallas as pl
from jax.experimental.pallas import tpu as pltpu
from jax.sharding import PartitionSpec as P

MESH = pl.DeviceIdType.MESH
F32 = jnp.float32
BF16 = jnp.bfloat16
SHARDS = 32
CAP = 64
D = 8192
CH = 256
NCH = 5
HEADS = (128, 208)
SQRT_HALF = 0.7071067811865476


def wait_for(ref, sem):
    pltpu.make_async_copy(ref, ref, sem).wait()


def send(src, dst, send_sem, recv_sem, device):
    pltpu.make_async_remote_copy(
        src_ref=src,
        dst_ref=dst,
        send_sem=send_sem,
        recv_sem=recv_sem,
        device_id=device,
        device_id_type=MESH,
    ).start()


def loop(name, count, step):
    with jax.named_scope(name):
        lax.fori_loop(0, count, step, 0)


def row_squares(values):
    ones = jnp.ones((8, values.shape[1]), F32)
    return lax.dot_general(
        ones,
        values,
        (((1,), (1,)), ((), ())),
        precision=lax.Precision.HIGHEST,
        preferred_element_type=F32,
    )


def merge_kernel(
    routing_hbm,
    pat_hbm,
    gain_hbm,
    nbias_hbm,
    w1_hbm,
    b1_hbm,
    w2_hbm,
    b2_hbm,
    text_hbm,
    img_out,
    tsums_out,
    isums_out,
    routing_ref,
    gain_ref,
    nbias_ref,
    b1_ref,
    b2_ref,
    pat,
    w1,
    nbuf,
    mer,
    hid,
    wbuf,
    stage,
    text,
    dsend,
    drecv,
    xsend,
    xrecv,
    fbuf,
    obuf,
    img,
    tbuf,
    ibuf,
    lsem,
    s_small,
    s0,
    s_first,
    s_stage,
    s_swap,
    s_w,
    s_p,
    s_p0,
    s_e,
    s_h,
    s_d,
    s_x,
    s_i,
    s_t,
    s_s,
    r_om,
    r_op,
    r_p,
    r_fm,
    r_fp,
    r_pm,
    r_pp,
    r_p2,
    r_h1,
    r_h2,
    r_h3,
    r_d,
    r_x,
    r_i,
    r_t,
    r_s,
):
    d = lax.axis_index("dp")
    t = lax.axis_index("tensor")
    z = lax.div(d, 8)
    y = lax.rem(lax.div(d, 2), 4)
    xl = lax.rem(d, 2)
    xh = lax.div(t, 2)
    c = lax.rem(t, 2)
    zp = lax.rem(z + 1, 4)
    zm = lax.rem(z + 3, 4)
    zo = lax.rem(z + 2, 4)
    yb = y + 1 - 2 * lax.rem(y, 2)
    q = xl + xh - 2 * xl * xh
    dev_zp = (zp * 8 + y * 2 + xl, t)
    dev_zm = (zm * 8 + y * 2 + xl, t)
    dev_ya = (z * 8 + (3 - y) * 2 + xl, t)
    dev_yb = (z * 8 + yb * 2 + xl, t)
    dev_x = (z * 8 + y * 2 + 1 - xl, t)
    dev_cut = (z * 8 + y * 2 + 1 - xl, (1 - xh) * 2 + c)
    dev_core = (d, xh * 2 + 1 - c)

    @pl.when(xh == 0)
    def _():
        pltpu.make_async_copy(w2_hbm, wbuf.at[z * 2], s_stage).start()

    @pl.when(xh == 1)
    def _():
        pltpu.make_async_copy(w2_hbm, stage, s_stage).start()

    pltpu.make_async_copy(pat_hbm, pat, lsem.at[NCH]).start()

    small = [
        pltpu.make_async_copy(src, dst, s_small.at[i])
        for i, (src, dst) in enumerate(
            (
                (routing_hbm, routing_ref),
                (gain_hbm, gain_ref),
                (nbias_hbm, nbias_ref),
                (b1_hbm, b1_ref),
                (b2_hbm, b2_ref),
            )
        )
    ]
    for copy in small:
        copy.start()

    barrier = pltpu.get_barrier_semaphore()
    base = d - lax.rem(d, 4)

    def greet(device):
        pl.semaphore_signal(barrier, inc=1, device_id=device, device_id_type=MESH)

    for o in range(-4, 8):
        other = lax.rem(base + o + SHARDS, SHARDS)

        @pl.when(other != d)
        def _():
            greet((other, t))

    greet(dev_zp)
    greet(dev_zm)
    greet(dev_cut)
    for i in range(1, 4):
        greet((d, lax.rem(t + i, 4)))

    for copy in small:
        copy.wait()

    width = pat.shape[1]
    gain = gain_ref[...].reshape(1, width)
    nbias = nbias_ref[...].reshape(1, width)

    def norm_pair(pair, carry):
        for u in range(2):
            norm_step(pair * 2 + u, nbuf.at[u])
        return carry

    def norm_step(step, nbuf):
        slot = lax.div(step, 4)
        part = lax.rem(step, 4)
        values = jnp.zeros((64, width), BF16)
        for b in range(4):
            start = pl.multiple_of(b * (4 * CAP) + part * 64, 64)
            chosen = (routing_ref[b, d] == slot).astype(F32).astype(BF16)
            values = values + pat[pl.ds(start, 64), :] * chosen
        values = values.astype(F32)
        centered = values - jnp.mean(values, axis=-1, keepdims=True)
        variance = jnp.mean(centered * centered, axis=-1, keepdims=True)
        normed = centered * lax.rsqrt(variance + 1e-06) * gain + nbias
        row = pl.multiple_of(step * 16, 16)
        for i in range(width // 128):
            nbuf[i] = normed[:, i * 128 : (i + 1) * 128]
        for j in range(4):
            for i in range(width // 128):
                mer[pl.ds(row, 16), j * width + i * 128 : j * width + (i + 1) * 128] = (
                    nbuf[i, pl.ds(j, 16, stride=4), :].astype(BF16)
                )

    with jax.named_scope("patches_in"):
        wait_for(pat, lsem.at[NCH])
    for n in range(NCH):
        pltpu.make_async_copy(
            w1_hbm.at[:, pl.ds(n * CH, CH)], w1.at[n], lsem.at[n]
        ).start()
    with jax.named_scope("norm_first"):
        lax.fori_loop(0, 2, norm_pair, 0)
    with jax.named_scope("greeting"):
        pl.semaphore_wait(barrier, 17)

    def own_send(kc, part=pl.ds(0, CH)):
        block = wbuf.at[z * 2, kc, part]
        send(block, block, s_w, r_om.at[kc], dev_zp)
        send(block, block, s_w, r_op.at[kc], dev_zm)
        send(block, wbuf.at[z * 2 + 1, kc, part], s_w, r_p.at[kc], dev_ya)

    with jax.named_scope("second_in"):
        wait_for(stage, s_stage)

    halves = (pl.ds(0, CH // 2), pl.ds(CH // 2, CH // 2))

    def swapped_half(half):
        with jax.named_scope("swapped"):
            wait_for(wbuf.at[z * 2, 0, halves[half]], s_first.at[half])
        own_send(0, halves[half])

    def swapped_send(kc):
        with jax.named_scope("swapped"):
            wait_for(wbuf.at[z * 2, kc], s0.at[kc])
        own_send(kc)

    @pl.when(xh == 1)
    def _():
        for half in range(2):
            send(
                stage.at[0, halves[half]],
                wbuf.at[z * 2, 0, halves[half]],
                s_swap,
                s_first.at[half],
                dev_x,
            )
        for kc in range(1, NCH):
            send(stage.at[kc], wbuf.at[z * 2, kc], s_swap, s0.at[kc], dev_x)

    @pl.when(xh == 0)
    def _():
        for kc in range(3):
            own_send(kc)

    with jax.named_scope("norm_rest"):
        lax.fori_loop(2, 8, norm_pair, 0)

    @pl.when(xh == 0)
    def _():
        own_send(3)
        own_send(4)

    @pl.when(xh == 1)
    def _():
        swapped_half(0)

    def hidden_step(n, carry):
        wait_for(w1.at[n], lsem.at[n])
        value = jnp.dot(mer[...], w1[n], preferred_element_type=F32)
        value = value + b1_ref[pl.ds(pl.multiple_of(n * CH, CH), CH)].reshape(1, CH)
        value = 0.5 * value * (1.0 + lax.erf(value * SQRT_HALF))
        hid[0, n] = value.astype(BF16)
        send(hid.at[0, n], hid.at[1, n], s_h, r_h1.at[n], dev_x)
        send(hid.at[0, n], hid.at[2, n], s_h, r_h2.at[n], dev_yb)

        @pl.when((xh == 1) & (n == 0))
        def _():
            swapped_half(1)

        @pl.when((xh == 1) & ((n == 2) | (n == 4)))
        def _():
            swapped_send(lax.div(n, 2))

        return carry

    loop("hidden_step", NCH, hidden_step)

    pltpu.make_async_copy(text_hbm, text, lsem.at[NCH + 1]).start()

    def far(kc):
        wait_for(wbuf.at[zm * 2, kc], r_om.at[kc])
        upper = wbuf.at[zm * 2, kc, pl.ds(0, CH // 2)]
        send(upper, upper, s_w, r_fm.at[kc], dev_zp)
        wait_for(wbuf.at[zp * 2, kc], r_op.at[kc])
        under = wbuf.at[zp * 2, kc, pl.ds(CH // 2, CH // 2)]
        send(under, under, s_w, r_fp.at[kc], dev_zm)

    def late_own(kc):
        @pl.when(xh == 1)
        def _():
            swapped_send(kc)

    def pair(kc):
        block = wbuf.at[z * 2 + 1, kc]
        wait_for(block, r_p.at[kc])
        if kc > 0:
            send(block, block, s_p, r_pm, dev_zp)
            send(block, block, s_p, r_pp, dev_zm)
        else:
            @pl.when(lax.div(z, 2) == xh)
            def _():
                send(block, block, s_p0, r_pm, dev_zp)
                send(block, block, s_p0, r_pp, dev_zm)

    def pair_first():
        for near, sem in ((zm, r_pm), (zp, r_pp)):

            @pl.when(lax.div(near, 2) != xh)
            def _():
                send(wbuf.at[near * 2, 0], wbuf.at[near * 2 + 1, 0], s_e, sem, dev_ya)

    def rows_x(n):
        wait_for(hid.at[1, n], r_h1.at[n])
        for half in range(2):

            @pl.when(xh == half)
            def _():
                top = pl.ds(0, HEADS[half])
                send(hid.at[1, n, top], hid.at[3, n, top], s_h, r_h3, dev_yb)

    def rows_y(n):
        wait_for(hid.at[2, n], r_h2.at[n])
        for half in range(2):

            @pl.when(xh == half)
            def _():
                rest = pl.ds(HEADS[half], CH - HEADS[half])
                send(hid.at[2, n, rest], hid.at[3, n, rest], s_h, r_h3, dev_x)

    def across_y(n):
        wait_for(wbuf.at[zo * 2, n, pl.ds(0, CH // 2)], r_fm.at[n])
        wait_for(wbuf.at[zo * 2, n, pl.ds(CH // 2, CH // 2)], r_fp.at[n])
        send(wbuf.at[zo * 2, n], wbuf.at[zo * 2 + 1, n], s_w, r_p2, dev_ya)

    def tile(rows, group, p):
        count = len(rows) * CH
        left = jnp.concatenate(
            [hid[rows[0] : rows[-1] + 1, n].reshape(count, CH) for n in range(NCH)],
            axis=1,
        )
        right = wbuf[group * 2 + p].reshape(NCH * CH, CH)
        return jnp.dot(left, right, preferred_element_type=F32)

    swap = lax.rem(z + c, 2)

    def pick(a, b, first):
        return a * first + b * (1 - first)

    def column_of(p):
        return (y + p * (3 - 2 * y)) * 2 + q

    def tiles(same, opposite):
        if same is None or opposite is None:
            to_z, to_p = my_z, my_p = opposite if same is None else same
        else:
            to_z = pick(same[0], opposite[0], swap)
            to_p = pick(same[1], opposite[1], swap)
            my_z = pick(opposite[0], same[0], swap)
            my_p = pick(opposite[1], same[1], swap)
        to_half = lax.rem(lax.div(to_z, 2) + xh + 1, 2)
        my_half = lax.rem(lax.div(my_z, 2) + xh + 1, 2)

        def give(rows):
            value = tile(rows, to_z, to_p).astype(BF16)

            def out():
                for i, r in enumerate(rows):
                    dsend[to_half, to_p, r] = value[i * CH : (i + 1) * CH]
                    send(
                        dsend.at[to_half, to_p, r],
                        drecv.at[to_half, to_p, r],
                        s_d,
                        r_d.at[to_half * 8 + to_p * 4 + r],
                        dev_core,
                    )

            return out

        def take(rows):
            value = tile(rows, my_z, my_p)

            def out():
                for i, r in enumerate(rows):
                    wait_for(
                        drecv.at[my_half, my_p, r], r_d.at[my_half * 8 + my_p * 4 + r]
                    )
                    mine = value[i * CH : (i + 1) * CH]
                    mine = mine + drecv[my_half, my_p, r].astype(F32)

                    @pl.when(my_half == 0)
                    def _():
                        xsend[my_p, r] = mine.astype(BF16)
                        there = r + 1 - 2 * (r % 2)
                        send(
                            xsend.at[my_p, r],
                            xrecv.at[my_p, there],
                            s_x,
                            r_x.at[my_p * 4 + there],
                            dev_cut,
                        )

                    @pl.when(my_half == 1)
                    def _():
                        column = pl.multiple_of(column_of(my_p) * CH, CH)
                        fbuf[my_p, r] = mine + b2_ref[:, pl.ds(column, CH)]

            return out

        return give, take

    near_a = tiles((z, 0), (zm, 0))
    near_b = tiles((z, 1), (zp, 0))
    middle = tiles((zo, 0), None)
    up = lax.rem(lax.div(zp, 2) + xh, 2)
    far_a = tiles((zo, 1), None)
    far_b = tiles(None, (pick(zp, zm, up), 1))
    far_c = tiles(None, (pick(zm, zp, up), 1))

    def give_near(r):
        with jax.named_scope(f"give_near{r}"):
            outs = [near_a[0]([r]), near_b[0]([r])]
            for out in outs:
                out()

    def take_near(r):
        with jax.named_scope(f"take_near{r}"):
            outs = [near_a[1]([r]), near_b[1]([r])]
            for out in outs:
                out()

    def run_single(name, steps, mine, rows):
        with jax.named_scope(name):

            @pl.when(swap != mine)
            def _():
                steps[0](rows)()

            @pl.when(swap == mine)
            def _():
                steps[1](rows)()

    def text_step(i, carry):
        rows = pl.ds(pl.multiple_of(i * CH, CH), CH)
        total = jnp.zeros((CH, CH), F32)
        for j in range(8):
            values = text[rows, j * CH : (j + 1) * CH].astype(F32)
            total = total + values * values
        tbuf[t, :, rows] = row_squares(total)
        return carry

    def share(buf, send_sems, recv_sems):
        for i in range(1, 4):
            send(
                buf.at[t],
                buf.at[t],
                send_sems.at[i - 1],
                recv_sems.at[i - 1],
                (d, lax.rem(t + i, 4)),
            )

    def step(label, work, *args):
        with jax.named_scope(label):
            work(*args)

    step("far0", far, 0)
    step("rows_y0", rows_y, 0)
    late_own(3)
    step("far1", far, 1)
    step("rows_y1", rows_y, 1)
    late_own(4)
    with jax.named_scope("text_in"):
        wait_for(text, lsem.at[NCH + 1])
    loop("text_step", 2, text_step)
    share(tbuf, s_t, r_t)
    step("far2", far, 2)
    step("rows_y2", rows_y, 2)
    step("rows_x0", rows_x, 0)
    step("across_y0", across_y, 0)
    step("far3", far, 3)
    step("rows_y3", rows_y, 3)
    step("across_y1", across_y, 1)
    step("rows_x1", rows_x, 1)
    step("rows_y4", rows_y, 4)
    step("far4", far, 4)
    for kc in range(NCH):
        step(f"pair{kc}", pair, kc)
    give_near(0)
    step("rows_x2", rows_x, 2)
    step("across_y2", across_y, 2)
    take_near(0)
    give_near(2)
    step("across_y3", across_y, 3)
    step("rows_x3", rows_x, 3)
    take_near(2)
    step("across_y4", across_y, 4)
    pair_first()
    run_single("middle", middle, 0, [0])
    step("rows_x4", rows_x, 4)
    give_near(1)
    run_single("middle", middle, 0, [1, 2])
    take_near(1)
    with jax.named_scope("diagonal"):
        wait_for(hid.at[3], r_h3)
    give_near(3)
    run_single("middle3", middle, 0, [3])
    take_near(3)

    def target(r, k):
        row_y = y + lax.div(r, 2) * (yb - y)
        row_x = xl + lax.rem(r, 2) * (1 - 2 * xl)
        return lax.rem(z * 8 + row_y * 2 + row_x + k, SHARDS)

    def pieces(p, r, k):
        rows = pl.ds(k * CAP, CAP)
        return obuf.at[p, r, rows], img.at[column_of(p), rows]

    def finish(p, r):
        with jax.named_scope(f"finish{p}{r}"):
            wait_for(xrecv.at[p, r], r_x.at[p * 4 + r])
            obuf[p, r] = (fbuf[p, r] + xrecv[p, r].astype(F32)).astype(BF16)
            for k in range(4):
                e = target(r, k)
                src, dst = pieces(p, r, k)

                @pl.when(e == d)
                def _():
                    pltpu.make_async_copy(src, dst, r_i).start()

                @pl.when((e != d) & (lax.div(e, 4) == lax.div(d, 4)))
                def _():
                    send(src, dst, s_i.at[p * 16 + r * 4 + k], r_i, (e, t))

    def onward(p, r):
        for k in range(1, 4):
            e = target(r, k)
            src, dst = pieces(p, r, k)

            @pl.when(lax.div(e, 4) != lax.div(d, 4))
            def _():
                send(src, dst, s_i.at[p * 16 + r * 4 + k], r_i, (e, t))

    def on_side(side, *work):
        @pl.when(xh == side)
        def _():
            for do, p, rows in work:
                for r in rows:
                    do(p, r)

    @pl.when((xh == 0) & (t != zo))
    def _():
        finish(0, 1)

    every = [0, 1, 2, 3]
    with jax.named_scope("pair_blocks_o"):
        wait_for(wbuf.at[zo * 2 + 1], r_p2)
    run_single("far_a", far_a, 0, every)

    @pl.when((xh == 0) & (t == zo))
    def _():
        finish(0, 1)

    on_side(0, (onward, 0, (1,)))
    on_side(1, (finish, 0, (1, 3, 0, 2)), (onward, 0, (1, 3, 0, 2)))
    with jax.named_scope("pair_blocks"):
        wait_for(wbuf.at[zm * 2 + 1], r_pm)
        wait_for(wbuf.at[zp * 2 + 1], r_pp)
    run_single("far_b", far_b, 1, every)
    on_side(0, (finish, 0, (3,)), (onward, 0, (3,)))
    run_single("far_c", far_c, 1, every)
    on_side(0, (finish, 0, (0,)), (onward, 0, (0,)))
    on_side(0, (finish, 0, (2,)), (onward, 0, (2,)))
    for r in (1, 0, 3, 2):
        finish(1, r)
        onward(1, r)

    with jax.named_scope("image_in"):
        wait_for(img, r_i)
    img_copy = pltpu.make_async_copy(img, img_out, lsem.at[0])
    img_copy.start()
    total = jnp.zeros((CH, CH), F32)
    for b in range(8):
        values = img[b].astype(F32)
        total = total + values * values
    ibuf[t] = row_squares(total)
    share(ibuf, s_s, r_s)
    for i in range(1, 4):
        wait_for(tbuf.at[lax.rem(t + 4 - i, 4)], r_t.at[i - 1])
    text_copy = pltpu.make_async_copy(tbuf, tsums_out, lsem.at[2])
    text_copy.start()
    with jax.named_scope("sums_in"):
        for i in range(1, 4):
            wait_for(ibuf.at[lax.rem(t + 4 - i, 4)], r_s.at[i - 1])
    sums_copy = pltpu.make_async_copy(ibuf, isums_out, lsem.at[1])
    sums_copy.start()

    wait_for(wbuf.at[pl.ds(0, 5)], s_w)
    wait_for(wbuf.at[pl.ds(0, 2), pl.ds(0, 4)], s_p)
    wait_for(wbuf.at[0, 0], s_e)

    @pl.when(lax.div(z, 2) == xh)
    def _():
        wait_for(wbuf.at[pl.ds(0, 2), 0], s_p0)

    @pl.when(xh == 1)
    def _():
        wait_for(wbuf.at[0], s_swap)

    wait_for(hid.at[pl.ds(0, 3)], s_h)
    wait_for(dsend, s_d)
    wait_for(xsend, s_x)
    for p in range(2):

        def drain(r, carry):
            for k in range(4):
                src, _unused = pieces(p, r, k)

                @pl.when(target(r, k) != d)
                def _():
                    wait_for(src, s_i.at[p * 16 + r * 4 + k])

            return carry

        loop("drain", 4, drain)
    for i in range(1, 4):
        wait_for(tbuf.at[t], s_t.at[i - 1])
        wait_for(ibuf.at[t], s_s.at[i - 1])
    img_copy.wait()
    text_copy.wait()
    sums_copy.wait()


def splice_kernel(
    grids_ref,
    routing_ref,
    text_hbm,
    img_hbm,
    tsums_hbm,
    isums_hbm,
    gain_hbm,
    emb_hbm,
    out_hbm,
    text,
    img,
    tsums,
    isums,
    gain,
    emb,
    out,
    in_sem,
    emb_sem,
    out_sem,
):
    rows = 128
    images = 4 * CAP
    steps = text.shape[0] // rows
    first = images // rows

    def part(ref, i):
        return ref.at[pl.ds(i * rows, rows)]

    small = [
        pltpu.make_async_copy(tsums_hbm, tsums, in_sem.at[steps]),
        pltpu.make_async_copy(isums_hbm, isums, in_sem.at[steps + 1]),
        pltpu.make_async_copy(gain_hbm, gain, in_sem.at[steps + 2]),
    ]
    whole = pltpu.make_async_copy(img_hbm, img, in_sem.at[steps + 3])
    order = list(range(first, steps)) + list(range(first))
    loads = {
        i: pltpu.make_async_copy(part(text_hbm, i), part(text, i), in_sem.at[i])
        for i in order
    }
    for copy in small[:1] + small[2:]:
        copy.start()
    for i in order[: steps - first]:
        loads[i].start()
    whole.start()
    small[1].start()
    for i in order[steps - first :]:
        loads[i].start()

    d = lax.axis_index("dp")
    starts = []
    total = jnp.int32(0)
    for k in range(4):
        s = lax.rem(d + SHARDS - k, SHARDS)
        count = jnp.int32(0)
        for b in range(4):
            size = grids_ref[b, 0, s] * grids_ref[b, 1, s]
            count = count + jnp.where(routing_ref[b, s] == k, size, 0)
        starts.append(total)
        total = total + count

    def picked(sums_ref, index):
        sums = sums_ref[0] + sums_ref[1] + sums_ref[2] + sums_ref[3]
        sums = sums[0:1, :]
        lanes = lax.broadcasted_iota(jnp.int32, (rows, sums.shape[1]), 1)
        return jnp.sum(jnp.where(lanes == index, sums, 0.0), axis=-1, keepdims=True)

    copies = []
    for copy in small[:1] + small[2:]:
        copy.wait()
    for i in order:
        position = i * rows + lax.broadcasted_iota(jnp.int32, (rows, 1), 0)
        square = picked(tsums, position)
        loads[i].wait()
        if i >= first:
            copies.append(
                pltpu.make_async_copy(part(text, i), part(emb_hbm, i), emb_sem.at[i])
            )
            copies[-1].start()
            scale = lax.rsqrt(square / D + 1e-06)
        else:
            if i == 0:
                whole.wait()
                small[1].wait()
            source = position
            for k in range(1, 4):
                shift = k * CAP - starts[k]
                if k > 1:
                    shift = shift - ((k - 1) * CAP - starts[k - 1])
                source = source + jnp.where(position >= starts[k], shift, 0)
            live = position < total
            square = jnp.where(live, picked(isums, source), square)
            scale = lax.rsqrt(square / D + 1e-06)
            picks = jnp.where(
                lax.broadcasted_iota(jnp.int32, (rows, images), 1) == source, 1.0, 0.0
            ).astype(BF16)
        here = slice(i * rows, (i + 1) * rows)
        for b in range(img.shape[0]):
            cols = slice(b * CH, (b + 1) * CH)
            value = text[here, cols].astype(F32)
            if i < first:
                taken = jnp.dot(picks, img[b], preferred_element_type=F32)
                value = jnp.where(live, taken, value)
                emb[here, cols] = value.astype(BF16)
            out[here, cols] = (value * scale * gain[:, cols]).astype(BF16)
        if i < first:
            copies.append(
                pltpu.make_async_copy(part(emb, i), part(emb_hbm, i), emb_sem.at[i])
            )
            copies[-1].start()
        copies.append(
            pltpu.make_async_copy(part(out, i), part(out_hbm, i), out_sem.at[i])
        )
        copies[-1].start()
    for copy in copies:
        copy.wait()


def per_device(
    patches,
    norm_gain,
    norm_bias,
    first_weight,
    first_bias,
    second_weight,
    second_bias,
    text_embeds,
    final_gain,
    image_grids,
    routing,
):
    seq, features = text_embeds.shape
    width = patches.shape[1]
    anywhere = pl.BlockSpec(memory_space=pl.ANY)
    smem = pl.BlockSpec(memory_space=pltpu.SMEM)
    dma = pltpu.SemaphoreType.DMA
    img, tsums, isums = pl.pallas_call(
        merge_kernel,
        out_shape=(
            jax.ShapeDtypeStruct((8, CH, CH), BF16),
            jax.ShapeDtypeStruct((4, 8, seq), F32),
            jax.ShapeDtypeStruct((4, 8, CH), F32),
        ),
        in_specs=[pl.BlockSpec(memory_space=pltpu.HBM)] * 9,
        out_specs=(anywhere, anywhere, anywhere),
        scratch_shapes=[
            pltpu.SMEM(routing.T.shape, jnp.int32),
            pltpu.VMEM(norm_gain.shape, F32),
            pltpu.VMEM(norm_bias.shape, F32),
            pltpu.VMEM(first_bias.shape, F32),
            pltpu.VMEM((1, second_bias.shape[0]), F32),
            pltpu.VMEM(patches.shape, BF16),
            pltpu.VMEM((NCH, first_weight.shape[0], CH), BF16),
            pltpu.VMEM((2, width // 128, 64, 128), F32),
            pltpu.VMEM((CH, 4 * width), BF16),
            pltpu.VMEM((4, NCH, CH, CH), BF16),
            pltpu.VMEM((8, NCH, CH, CH), BF16),
            pltpu.VMEM((NCH, CH, CH), BF16),
            pltpu.VMEM((seq, features), BF16),
            pltpu.VMEM((2, 2, 4, CH, CH), BF16),
            pltpu.VMEM((2, 2, 4, CH, CH), BF16),
            pltpu.VMEM((2, 4, CH, CH), BF16),
            pltpu.VMEM((2, 4, CH, CH), BF16),
            pltpu.VMEM((2, 4, CH, CH), F32),
            pltpu.VMEM((2, 4, CH, CH), BF16),
            pltpu.VMEM((8, CH, CH), BF16),
            pltpu.VMEM((4, 8, seq), F32),
            pltpu.VMEM((4, 8, CH), F32),
            dma((NCH + 2,)),
            dma((5,)),
            dma((NCH,)),
            dma((2,)),
            dma,
            dma,
            dma,
            dma,
            dma,
            dma,
            dma,
            dma,
            dma,
            dma((32,)),
            dma((3,)),
            dma((3,)),
            dma((NCH,)),
            dma((NCH,)),
            dma((NCH,)),
            dma((NCH,)),
            dma((NCH,)),
            dma,
            dma,
            dma,
            dma((NCH,)),
            dma((NCH,)),
            dma,
            dma((16,)),
            dma((8,)),
            dma,
            dma((3,)),
            dma((3,)),
        ],
        compiler_params=pltpu.CompilerParams(
            collective_id=0, has_side_effects=True, vmem_limit_bytes=60 * 1024 * 1024
        ),
        name="merge",
    )(
        routing.T,
        patches,
        norm_gain,
        norm_bias,
        first_weight,
        first_bias,
        second_weight.reshape(NCH, CH, CH),
        second_bias.reshape(1, -1),
        text_embeds,
    )
    return pl.pallas_call(
        splice_kernel,
        out_shape=(
            jax.ShapeDtypeStruct((seq, features), BF16),
            jax.ShapeDtypeStruct((seq, features), BF16),
        ),
        in_specs=[smem, smem] + [anywhere] * 5,
        out_specs=(anywhere, anywhere),
        scratch_shapes=[
            pltpu.VMEM((seq, features), BF16),
            pltpu.VMEM(img.shape, BF16),
            pltpu.VMEM(tsums.shape, F32),
            pltpu.VMEM(isums.shape, F32),
            pltpu.VMEM((1, features), F32),
            pltpu.VMEM((4 * CAP, features), BF16),
            pltpu.VMEM((seq, features), BF16),
            dma((8,)),
            dma((4,)),
            dma((4,)),
        ],
        compiler_params=pltpu.CompilerParams(vmem_limit_bytes=60 * 1024 * 1024),
        name="splice",
    )(
        image_grids.transpose(1, 2, 0),
        routing.T,
        text_embeds,
        img,
        tsums,
        isums,
        final_gain.reshape(1, -1),
    )


def solution(mesh):
    placed = (
        P("dp", None),
        P(),
        P(),
        P(None, "tensor"),
        P("tensor"),
        P("tensor", "dp"),
        P("tensor"),
        P("dp", "tensor"),
        P("tensor"),
        P(),
        P(),
    )
    return jax.shard_map(
        per_device,
        mesh=mesh,
        in_specs=placed,
        out_specs=(P("dp", "tensor"), P("dp", "tensor")),
        check_vma=False,
    )
```

```python
import functools

import jax
import jax.numpy as jnp
from jax import lax
from jax.experimental import pallas as pl
from jax.experimental.pallas import tpu as pltpu
from jax.sharding import PartitionSpec as P

MESH = pl.DeviceIdType.MESH
F32 = jnp.float32
BF16 = jnp.bfloat16
SHARDS = 32
CAP = 64
D = 8192
CH = 256
NCH = 5
HEADS = (128, 208)
SQRT_HALF = 0.7071067811865476


def wait_for(ref, sem):
    pltpu.make_async_copy(ref, ref, sem).wait()


def send(src, dst, send_sem, recv_sem, device):
    pltpu.make_async_remote_copy(
        src_ref=src,
        dst_ref=dst,
        send_sem=send_sem,
        recv_sem=recv_sem,
        device_id=device,
        device_id_type=MESH,
    ).start()


def loop(name, count, step):
    with jax.named_scope(name):
        lax.fori_loop(0, count, step, 0)


def row_squares(values):
    ones = jnp.ones((8, values.shape[1]), F32)
    return lax.dot_general(
        ones,
        values,
        (((1,), (1,)), ((), ())),
        precision=lax.Precision.HIGHEST,
        preferred_element_type=F32,
    )


def merge_kernel(
    routing_hbm,
    pat_hbm,
    gain_hbm,
    nbias_hbm,
    w1_hbm,
    b1_hbm,
    w2_hbm,
    b2_hbm,
    text_hbm,
    img_out,
    tsums_out,
    isums_out,
    routing_ref,
    gain_ref,
    nbias_ref,
    b1_ref,
    b2_ref,
    pat,
    w1,
    nbuf,
    mer,
    hid,
    wbuf,
    stage,
    text,
    dsend,
    drecv,
    xsend,
    xrecv,
    fbuf,
    obuf,
    img,
    tbuf,
    ibuf,
    lsem,
    s_small,
    s0,
    s_first,
    s_stage,
    s_swap,
    s_w,
    s_p,
    s_p0,
    s_e,
    s_h,
    s_d,
    s_x,
    s_i,
    s_t,
    s_s,
    r_om,
    r_op,
    r_p,
    r_fm,
    r_fp,
    r_pm,
    r_pp,
    r_p2,
    r_h1,
    r_h2,
    r_h3,
    r_d,
    r_x,
    r_i,
    r_t,
    r_s,
):
    d = lax.axis_index("dp")
    t = lax.axis_index("tensor")
    z = lax.div(d, 8)
    y = lax.rem(lax.div(d, 2), 4)
    xl = lax.rem(d, 2)
    xh = lax.div(t, 2)
    c = lax.rem(t, 2)
    zp = lax.rem(z + 1, 4)
    zm = lax.rem(z + 3, 4)
    zo = lax.rem(z + 2, 4)
    yb = y + 1 - 2 * lax.rem(y, 2)
    q = xl + xh - 2 * xl * xh
    dev_zp = (zp * 8 + y * 2 + xl, t)
    dev_zm = (zm * 8 + y * 2 + xl, t)
    dev_ya = (z * 8 + (3 - y) * 2 + xl, t)
    dev_yb = (z * 8 + yb * 2 + xl, t)
    dev_x = (z * 8 + y * 2 + 1 - xl, t)
    dev_cut = (z * 8 + y * 2 + 1 - xl, (1 - xh) * 2 + c)
    dev_core = (d, xh * 2 + 1 - c)

    @pl.when(xh == 0)
    def _():
        pltpu.make_async_copy(w2_hbm, wbuf.at[z * 2], s_stage).start()

    @pl.when(xh == 1)
    def _():
        pltpu.make_async_copy(w2_hbm, stage, s_stage).start()

    pltpu.make_async_copy(pat_hbm, pat, lsem.at[NCH]).start()

    small = [
        pltpu.make_async_copy(src, dst, s_small.at[i])
        for i, (src, dst) in enumerate(
            (
                (routing_hbm, routing_ref),
                (gain_hbm, gain_ref),
                (nbias_hbm, nbias_ref),
                (b1_hbm, b1_ref),
                (b2_hbm, b2_ref),
            )
        )
    ]
    for copy in small:
        copy.start()

    barrier = pltpu.get_barrier_semaphore()
    base = d - lax.rem(d, 4)

    def greet(device):
        pl.semaphore_signal(barrier, inc=1, device_id=device, device_id_type=MESH)

    for o in range(-4, 8):
        other = lax.rem(base + o + SHARDS, SHARDS)

        @pl.when(other != d)
        def _():
            greet((other, t))

    greet(dev_zp)
    greet(dev_zm)
    greet(dev_cut)
    for i in range(1, 4):
        greet((d, lax.rem(t + i, 4)))

    for copy in small:
        copy.wait()

    width = pat.shape[1]
    gain = gain_ref[...].reshape(1, width)
    nbias = nbias_ref[...].reshape(1, width)

    def norm_pair(pair, carry):
        for u in range(2):
            norm_step(pair * 2 + u, nbuf.at[u])
        return carry

    def norm_step(step, nbuf):
        slot = lax.div(step, 4)
        part = lax.rem(step, 4)
        values = jnp.zeros((64, width), BF16)
        for b in range(4):
            start = pl.multiple_of(b * (4 * CAP) + part * 64, 64)
            chosen = (routing_ref[b, d] == slot).astype(F32).astype(BF16)
            values = values + pat[pl.ds(start, 64), :] * chosen
        values = values.astype(F32)
        centered = values - jnp.mean(values, axis=-1, keepdims=True)
        variance = jnp.mean(centered * centered, axis=-1, keepdims=True)
        normed = centered * lax.rsqrt(variance + 1e-06) * gain + nbias
        row = pl.multiple_of(step * 16, 16)
        for i in range(width // 128):
            nbuf[i] = normed[:, i * 128 : (i + 1) * 128]
        for j in range(4):
            for i in range(width // 128):
                mer[pl.ds(row, 16), j * width + i * 128 : j * width + (i + 1) * 128] = (
                    nbuf[i, pl.ds(j, 16, stride=4), :].astype(BF16)
                )

    with jax.named_scope("patches_in"):
        wait_for(pat, lsem.at[NCH])
    for n in range(NCH):
        pltpu.make_async_copy(
            w1_hbm.at[:, pl.ds(n * CH, CH)], w1.at[n], lsem.at[n]
        ).start()
    with jax.named_scope("norm_first"):
        lax.fori_loop(0, 2, norm_pair, 0)
    with jax.named_scope("greeting"):
        pl.semaphore_wait(barrier, 17)

    def own_send(kc, part=pl.ds(0, CH)):
        block = wbuf.at[z * 2, kc, part]
        send(block, block, s_w, r_om.at[kc], dev_zp)
        send(block, block, s_w, r_op.at[kc], dev_zm)
        send(block, wbuf.at[z * 2 + 1, kc, part], s_w, r_p.at[kc], dev_ya)

    with jax.named_scope("second_in"):
        wait_for(stage, s_stage)

    halves = (pl.ds(0, CH // 2), pl.ds(CH // 2, CH // 2))

    def swapped_half(half):
        with jax.named_scope("swapped"):
            wait_for(wbuf.at[z * 2, 0, halves[half]], s_first.at[half])
        own_send(0, halves[half])

    def swapped_send(kc):
        with jax.named_scope("swapped"):
            wait_for(wbuf.at[z * 2, kc], s0.at[kc])
        own_send(kc)

    @pl.when(xh == 1)
    def _():
        for half in range(2):
            send(
                stage.at[0, halves[half]],
                wbuf.at[z * 2, 0, halves[half]],
                s_swap,
                s_first.at[half],
                dev_x,
            )
        for kc in range(1, NCH):
            send(stage.at[kc], wbuf.at[z * 2, kc], s_swap, s0.at[kc], dev_x)

    @pl.when(xh == 0)
    def _():
        for kc in range(3):
            own_send(kc)

    with jax.named_scope("norm_rest"):
        lax.fori_loop(2, 8, norm_pair, 0)

    @pl.when(xh == 0)
    def _():
        own_send(3)
        own_send(4)

    @pl.when(xh == 1)
    def _():
        swapped_half(0)

    def hidden_step(n, carry):
        wait_for(w1.at[n], lsem.at[n])
        value = jnp.dot(mer[...], w1[n], preferred_element_type=F32)
        value = value + b1_ref[pl.ds(pl.multiple_of(n * CH, CH), CH)].reshape(1, CH)
        value = 0.5 * value * (1.0 + lax.erf(value * SQRT_HALF))
        hid[0, n] = value.astype(BF16)
        send(hid.at[0, n], hid.at[1, n], s_h, r_h1.at[n], dev_x)
        send(hid.at[0, n], hid.at[2, n], s_h, r_h2.at[n], dev_yb)

        @pl.when((xh == 1) & (n == 0))
        def _():
            swapped_half(1)

        @pl.when((xh == 1) & ((n == 2) | (n == 4)))
        def _():
            swapped_send(lax.div(n, 2))

        return carry

    loop("hidden_step", NCH, hidden_step)

    pltpu.make_async_copy(text_hbm, text, lsem.at[NCH + 1]).start()

    def far(kc):
        wait_for(wbuf.at[zm * 2, kc], r_om.at[kc])
        upper = wbuf.at[zm * 2, kc, pl.ds(0, CH // 2)]
        send(upper, upper, s_w, r_fm.at[kc], dev_zp)
        wait_for(wbuf.at[zp * 2, kc], r_op.at[kc])
        under = wbuf.at[zp * 2, kc, pl.ds(CH // 2, CH // 2)]
        send(under, under, s_w, r_fp.at[kc], dev_zm)

    def late_own(kc):
        @pl.when(xh == 1)
        def _():
            swapped_send(kc)

    def pair(kc):
        block = wbuf.at[z * 2 + 1, kc]
        wait_for(block, r_p.at[kc])
        if kc > 0:
            send(block, block, s_p, r_pm, dev_zp)
            send(block, block, s_p, r_pp, dev_zm)
        else:
            @pl.when(lax.div(z, 2) == xh)
            def _():
                send(block, block, s_p0, r_pm, dev_zp)
                send(block, block, s_p0, r_pp, dev_zm)

    def pair_first():
        for near, sem in ((zm, r_pm), (zp, r_pp)):

            @pl.when(lax.div(near, 2) != xh)
            def _():
                send(wbuf.at[near * 2, 0], wbuf.at[near * 2 + 1, 0], s_e, sem, dev_ya)

    def rows_x(n):
        wait_for(hid.at[1, n], r_h1.at[n])
        for half in range(2):

            @pl.when(xh == half)
            def _():
                top = pl.ds(0, HEADS[half])
                send(hid.at[1, n, top], hid.at[3, n, top], s_h, r_h3, dev_yb)

    def rows_y(n):
        wait_for(hid.at[2, n], r_h2.at[n])
        for half in range(2):

            @pl.when(xh == half)
            def _():
                rest = pl.ds(HEADS[half], CH - HEADS[half])
                send(hid.at[2, n, rest], hid.at[3, n, rest], s_h, r_h3, dev_x)

    def across_y(n):
        wait_for(wbuf.at[zo * 2, n, pl.ds(0, CH // 2)], r_fm.at[n])
        wait_for(wbuf.at[zo * 2, n, pl.ds(CH // 2, CH // 2)], r_fp.at[n])
        send(wbuf.at[zo * 2, n], wbuf.at[zo * 2 + 1, n], s_w, r_p2, dev_ya)

    def tile(rows, group, p):
        count = len(rows) * CH
        left = jnp.concatenate(
            [hid[rows[0] : rows[-1] + 1, n].reshape(count, CH) for n in range(NCH)],
            axis=1,
        )
        right = wbuf[group * 2 + p].reshape(NCH * CH, CH)
        return jnp.dot(left, right, preferred_element_type=F32)

    swap = lax.rem(z + c, 2)

    def pick(a, b, first):
        return a * first + b * (1 - first)

    def column_of(p):
        return (y + p * (3 - 2 * y)) * 2 + q

    def tiles(same, opposite):
        if same is None or opposite is None:
            to_z, to_p = my_z, my_p = opposite if same is None else same
        else:
            to_z = pick(same[0], opposite[0], swap)
            to_p = pick(same[1], opposite[1], swap)
            my_z = pick(opposite[0], same[0], swap)
            my_p = pick(opposite[1], same[1], swap)
        to_half = lax.rem(lax.div(to_z, 2) + xh + 1, 2)
        my_half = lax.rem(lax.div(my_z, 2) + xh + 1, 2)

        def give(rows):
            value = tile(rows, to_z, to_p).astype(BF16)

            def out():
                for i, r in enumerate(rows):
                    dsend[to_half, to_p, r] = value[i * CH : (i + 1) * CH]
                    send(
                        dsend.at[to_half, to_p, r],
                        drecv.at[to_half, to_p, r],
                        s_d,
                        r_d.at[to_half * 8 + to_p * 4 + r],
                        dev_core,
                    )

            return out

        def take(rows):
            value = tile(rows, my_z, my_p)

            def out():
                for i, r in enumerate(rows):
                    wait_for(
                        drecv.at[my_half, my_p, r], r_d.at[my_half * 8 + my_p * 4 + r]
                    )
                    mine = value[i * CH : (i + 1) * CH]
                    mine = mine + drecv[my_half, my_p, r].astype(F32)

                    @pl.when(my_half == 0)
                    def _():
                        xsend[my_p, r] = mine.astype(BF16)
                        there = r + 1 - 2 * (r % 2)
                        send(
                            xsend.at[my_p, r],
                            xrecv.at[my_p, there],
                            s_x,
                            r_x.at[my_p * 4 + there],
                            dev_cut,
                        )

                    @pl.when(my_half == 1)
                    def _():
                        column = pl.multiple_of(column_of(my_p) * CH, CH)
                        fbuf[my_p, r] = mine + b2_ref[:, pl.ds(column, CH)]

            return out

        return give, take

    near_a = tiles((z, 0), (zm, 0))
    near_b = tiles((z, 1), (zp, 0))
    middle = tiles((zo, 0), None)
    up = lax.rem(lax.div(zp, 2) + xh, 2)
    far_a = tiles((zo, 1), None)
    far_b = tiles(None, (pick(zp, zm, up), 1))
    far_c = tiles(None, (pick(zm, zp, up), 1))

    def give_near(r):
        with jax.named_scope(f"give_near{r}"):
            outs = [near_a[0]([r]), near_b[0]([r])]
            for out in outs:
                out()

    def take_near(r):
        with jax.named_scope(f"take_near{r}"):
            outs = [near_a[1]([r]), near_b[1]([r])]
            for out in outs:
                out()

    def run_single(name, steps, mine, rows):
        with jax.named_scope(name):

            @pl.when(swap != mine)
            def _():
                steps[0](rows)()

            @pl.when(swap == mine)
            def _():
                steps[1](rows)()

    def text_step(i, carry):
        rows = pl.ds(pl.multiple_of(i * CH, CH), CH)
        total = jnp.zeros((CH, CH), F32)
        for j in range(8):
            values = text[rows, j * CH : (j + 1) * CH].astype(F32)
            total = total + values * values
        tbuf[:, rows] = row_squares(total)
        return carry

    def share(buf, result, own_sem, send_sems, recv_sems):
        pltpu.make_async_copy(buf, result.at[t], own_sem).start()
        for i in range(1, 4):
            send(
                buf,
                result.at[t],
                send_sems.at[i - 1],
                recv_sems.at[i - 1],
                (d, lax.rem(t + i, 4)),
            )

    def step(label, work, *args):
        with jax.named_scope(label):
            work(*args)

    def target(r, k):
        row_y = y + lax.div(r, 2) * (yb - y)
        row_x = xl + lax.rem(r, 2) * (1 - 2 * xl)
        return lax.rem(z * 8 + row_y * 2 + row_x + k, SHARDS)

    def pieces(p, r, k):
        rows = pl.ds(k * CAP, CAP)
        return obuf.at[p, r, rows], img.at[column_of(p), rows]

    def finish(p, r):
        with jax.named_scope(f"finish{p}{r}"):
            wait_for(xrecv.at[p, r], r_x.at[p * 4 + r])
            obuf[p, r] = (fbuf[p, r] + xrecv[p, r].astype(F32)).astype(BF16)
            for k in range(4):
                e = target(r, k)
                src, dst = pieces(p, r, k)

                @pl.when(e == d)
                def _():
                    pltpu.make_async_copy(src, dst, r_i).start()

                @pl.when((e != d) & (lax.div(e, 4) == lax.div(d, 4)))
                def _():
                    send(src, dst, s_i.at[p * 16 + r * 4 + k], r_i, (e, t))

    def onward(p, r):
        for k in range(1, 4):
            e = target(r, k)
            src, dst = pieces(p, r, k)

            @pl.when(lax.div(e, 4) != lax.div(d, 4))
            def _():
                send(src, dst, s_i.at[p * 16 + r * 4 + k], r_i, (e, t))

    def on_side(side, *work):
        @pl.when(xh == side)
        def _():
            for do, p, rows in work:
                for r in rows:
                    do(p, r)

    step("far0", far, 0)
    step("rows_y0", rows_y, 0)
    late_own(3)
    step("far1", far, 1)
    step("rows_y1", rows_y, 1)
    late_own(4)
    with jax.named_scope("text_in"):
        wait_for(text, lsem.at[NCH + 1])
    loop("text_step", 2, text_step)
    share(tbuf, tsums_out, lsem.at[2], s_t, r_t)
    step("far2", far, 2)
    step("rows_y2", rows_y, 2)
    step("rows_x0", rows_x, 0)
    step("across_y0", across_y, 0)
    step("far3", far, 3)
    step("rows_y3", rows_y, 3)
    step("across_y1", across_y, 1)
    step("rows_x1", rows_x, 1)
    step("rows_y4", rows_y, 4)
    step("far4", far, 4)
    for kc in range(NCH):
        step(f"pair{kc}", pair, kc)
    give_near(0)
    step("rows_x2", rows_x, 2)
    step("across_y2", across_y, 2)
    take_near(0)
    give_near(2)
    step("across_y3", across_y, 3)
    step("rows_x3", rows_x, 3)
    take_near(2)
    step("across_y4", across_y, 4)
    pair_first()
    run_single("middle", middle, 0, [0])
    step("rows_x4", rows_x, 4)
    give_near(1)
    run_single("middle", middle, 0, [1, 2])
    take_near(1)
    with jax.named_scope("diagonal"):
        wait_for(hid.at[3], r_h3)
    on_side(1, (finish, 0, (1, 0)))
    give_near(3)
    run_single("middle3", middle, 0, [3])
    take_near(3)

    @pl.when((xh == 0) & (t != zo))
    def _():
        finish(0, 1)

    every = [0, 1, 2, 3]
    with jax.named_scope("pair_blocks_o"):
        wait_for(wbuf.at[zo * 2 + 1], r_p2)
    run_single("far_a", far_a, 0, every)

    @pl.when((xh == 0) & (t == zo))
    def _():
        finish(0, 1)

    on_side(0, (onward, 0, (1,)))
    on_side(1, (onward, 0, (1, 0)), (finish, 0, (3, 2)), (onward, 0, (3, 2)))
    with jax.named_scope("pair_blocks"):
        wait_for(wbuf.at[zm * 2 + 1], r_pm)
        wait_for(wbuf.at[zp * 2 + 1], r_pp)
    run_single("far_b", far_b, 1, every)
    on_side(0, (finish, 0, (3,)), (onward, 0, (3,)))
    run_single("far_c", far_c, 1, every)
    on_side(0, (finish, 0, (0,)), (onward, 0, (0,)))
    on_side(0, (finish, 0, (2,)), (onward, 0, (2,)))
    for r in (1, 0, 3, 2):
        finish(1, r)
        onward(1, r)

    with jax.named_scope("image_in"):
        wait_for(img, r_i)
    img_copy = pltpu.make_async_copy(img, img_out, lsem.at[0])
    img_copy.start()
    total = jnp.zeros((CH, CH), F32)
    for b in range(8):
        values = img[b].astype(F32)
        total = total + values * values
    ibuf[...] = row_squares(total)
    share(ibuf, isums_out, lsem.at[1], s_s, r_s)
    for i in range(1, 4):
        wait_for(tsums_out.at[lax.rem(t + 4 - i, 4)], r_t.at[i - 1])
    wait_for(tbuf, lsem.at[2])
    with jax.named_scope("sums_in"):
        for i in range(1, 4):
            wait_for(isums_out.at[lax.rem(t + 4 - i, 4)], r_s.at[i - 1])
    wait_for(ibuf, lsem.at[1])

    wait_for(wbuf.at[pl.ds(0, 5)], s_w)
    wait_for(wbuf.at[pl.ds(0, 2), pl.ds(0, 4)], s_p)
    wait_for(wbuf.at[0, 0], s_e)

    @pl.when(lax.div(z, 2) == xh)
    def _():
        wait_for(wbuf.at[pl.ds(0, 2), 0], s_p0)

    @pl.when(xh == 1)
    def _():
        wait_for(wbuf.at[0], s_swap)

    wait_for(hid.at[pl.ds(0, 3)], s_h)
    wait_for(dsend, s_d)
    wait_for(xsend, s_x)
    for p in range(2):

        def drain(r, carry):
            for k in range(4):
                src, _unused = pieces(p, r, k)

                @pl.when(target(r, k) != d)
                def _():
                    wait_for(src, s_i.at[p * 16 + r * 4 + k])

            return carry

        loop("drain", 4, drain)
    for i in range(1, 4):
        wait_for(tbuf, s_t.at[i - 1])
        wait_for(ibuf, s_s.at[i - 1])
    img_copy.wait()


def splice_kernel(
    grids_hbm,
    routing_hbm,
    text_hbm,
    img_hbm,
    tsums_hbm,
    isums_hbm,
    gain_hbm,
    emb_hbm,
    out_hbm,
    grids_ref,
    routing_ref,
    text,
    img,
    tsums,
    isums,
    gain,
    emb,
    out,
    in_sem,
    emb_sem,
    out_sem,
):
    rows = 128
    images = 4 * CAP
    steps = text.shape[0] // rows
    first = images // rows

    def part(ref, i):
        return ref.at[pl.ds(i * rows, rows)]

    small = [
        pltpu.make_async_copy(tsums_hbm, tsums, in_sem.at[steps]),
        pltpu.make_async_copy(isums_hbm, isums, in_sem.at[steps + 1]),
        pltpu.make_async_copy(gain_hbm, gain, in_sem.at[steps + 2]),
    ]
    whole = pltpu.make_async_copy(img_hbm, img, in_sem.at[steps + 3])
    order = list(range(first, steps)) + list(range(first))
    loads = {
        i: pltpu.make_async_copy(part(text_hbm, i), part(text, i), in_sem.at[i])
        for i in order
    }
    for copy in small[:1] + small[2:]:
        copy.start()
    for i in order[: steps - first]:
        loads[i].start()
    whole.start()
    small[1].start()
    tables = [
        pltpu.make_async_copy(grids_hbm, grids_ref, in_sem.at[steps + 4]),
        pltpu.make_async_copy(routing_hbm, routing_ref, in_sem.at[steps + 5]),
    ]
    for copy in tables:
        copy.start()
    for i in order[steps - first :]:
        loads[i].start()

    d = lax.axis_index("dp")
    for copy in tables:
        copy.wait()
    starts = []
    total = jnp.int32(0)
    for k in range(4):
        s = lax.rem(d + SHARDS - k, SHARDS)
        count = jnp.int32(0)
        for b in range(4):
            size = grids_ref[b, 0, s] * grids_ref[b, 1, s]
            count = count + jnp.where(routing_ref[b, s] == k, size, 0)
        starts.append(total)
        total = total + count

    def picked(sums_ref, index):
        sums = sums_ref[0] + sums_ref[1] + sums_ref[2] + sums_ref[3]
        sums = sums[0:1, :]
        lanes = lax.broadcasted_iota(jnp.int32, (rows, sums.shape[1]), 1)
        return jnp.sum(jnp.where(lanes == index, sums, 0.0), axis=-1, keepdims=True)

    copies = []
    for copy in small[:1] + small[2:]:
        copy.wait()
    for i in order:
        position = i * rows + lax.broadcasted_iota(jnp.int32, (rows, 1), 0)
        square = picked(tsums, position)
        loads[i].wait()
        if i >= first:
            copies.append(
                pltpu.make_async_copy(part(text, i), part(emb_hbm, i), emb_sem.at[i])
            )
            copies[-1].start()
            scale = lax.rsqrt(square / D + 1e-06)
        else:
            if i == 0:
                whole.wait()
                small[1].wait()
            source = position
            for k in range(1, 4):
                shift = k * CAP - starts[k]
                if k > 1:
                    shift = shift - ((k - 1) * CAP - starts[k - 1])
                source = source + jnp.where(position >= starts[k], shift, 0)
            live = position < total
            square = jnp.where(live, picked(isums, source), square)
            scale = lax.rsqrt(square / D + 1e-06)
            picks = jnp.where(
                lax.broadcasted_iota(jnp.int32, (rows, images), 1) == source, 1.0, 0.0
            ).astype(BF16)
        here = slice(i * rows, (i + 1) * rows)
        for b in range(img.shape[0]):
            cols = slice(b * CH, (b + 1) * CH)
            value = text[here, cols].astype(F32)
            if i < first:
                taken = jnp.dot(picks, img[b], preferred_element_type=F32)
                value = jnp.where(live, taken, value)
                emb[here, cols] = value.astype(BF16)
            out[here, cols] = (value * scale * gain[:, cols]).astype(BF16)
        if i < first:
            copies.append(
                pltpu.make_async_copy(part(emb, i), part(emb_hbm, i), emb_sem.at[i])
            )
            copies[-1].start()
        copies.append(
            pltpu.make_async_copy(part(out, i), part(out_hbm, i), out_sem.at[i])
        )
        copies[-1].start()
    for copy in copies:
        copy.wait()


def per_device(
    patches,
    norm_gain,
    norm_bias,
    first_weight,
    first_bias,
    second_weight,
    second_bias,
    text_embeds,
    final_gain,
    image_grids,
    routing,
):
    seq, features = text_embeds.shape
    width = patches.shape[1]
    anywhere = pl.BlockSpec(memory_space=pl.ANY)
    dma = pltpu.SemaphoreType.DMA
    img, tsums, isums = pl.pallas_call(
        merge_kernel,
        out_shape=(
            jax.ShapeDtypeStruct((8, CH, CH), BF16),
            jax.ShapeDtypeStruct((4, 8, seq), F32),
            jax.ShapeDtypeStruct((4, 8, CH), F32),
        ),
        in_specs=[pl.BlockSpec(memory_space=pltpu.HBM)] * 9,
        out_specs=(anywhere, anywhere, anywhere),
        scratch_shapes=[
            pltpu.SMEM(routing.T.shape, jnp.int32),
            pltpu.VMEM(norm_gain.shape, F32),
            pltpu.VMEM(norm_bias.shape, F32),
            pltpu.VMEM(first_bias.shape, F32),
            pltpu.VMEM((1, second_bias.shape[0]), F32),
            pltpu.VMEM(patches.shape, BF16),
            pltpu.VMEM((NCH, first_weight.shape[0], CH), BF16),
            pltpu.VMEM((2, width // 128, 64, 128), F32),
            pltpu.VMEM((CH, 4 * width), BF16),
            pltpu.VMEM((4, NCH, CH, CH), BF16),
            pltpu.VMEM((8, NCH, CH, CH), BF16),
            pltpu.VMEM((NCH, CH, CH), BF16),
            pltpu.VMEM((seq, features), BF16),
            pltpu.VMEM((2, 2, 4, CH, CH), BF16),
            pltpu.VMEM((2, 2, 4, CH, CH), BF16),
            pltpu.VMEM((2, 4, CH, CH), BF16),
            pltpu.VMEM((2, 4, CH, CH), BF16),
            pltpu.VMEM((2, 4, CH, CH), F32),
            pltpu.VMEM((2, 4, CH, CH), BF16),
            pltpu.VMEM((8, CH, CH), BF16),
            pltpu.VMEM((8, seq), F32),
            pltpu.VMEM((8, CH), F32),
            dma((NCH + 2,)),
            dma((5,)),
            dma((NCH,)),
            dma((2,)),
            dma,
            dma,
            dma,
            dma,
            dma,
            dma,
            dma,
            dma,
            dma,
            dma((32,)),
            dma((3,)),
            dma((3,)),
            dma((NCH,)),
            dma((NCH,)),
            dma((NCH,)),
            dma((NCH,)),
            dma((NCH,)),
            dma,
            dma,
            dma,
            dma((NCH,)),
            dma((NCH,)),
            dma,
            dma((16,)),
            dma((8,)),
            dma,
            dma((3,)),
            dma((3,)),
        ],
        compiler_params=pltpu.CompilerParams(
            collective_id=0, has_side_effects=True, vmem_limit_bytes=60 * 1024 * 1024
        ),
        name="merge",
    )(
        routing.T,
        patches,
        norm_gain,
        norm_bias,
        first_weight,
        first_bias,
        second_weight.reshape(NCH, CH, CH),
        second_bias.reshape(1, -1),
        text_embeds,
    )
    return pl.pallas_call(
        splice_kernel,
        out_shape=(
            jax.ShapeDtypeStruct((seq, features), BF16),
            jax.ShapeDtypeStruct((seq, features), BF16),
        ),
        in_specs=[anywhere] * 7,
        out_specs=(anywhere, anywhere),
        scratch_shapes=[
            pltpu.SMEM((image_grids.shape[1], 2, SHARDS), jnp.int32),
            pltpu.SMEM(routing.T.shape, jnp.int32),
            pltpu.VMEM((seq, features), BF16),
            pltpu.VMEM(img.shape, BF16),
            pltpu.VMEM(tsums.shape, F32),
            pltpu.VMEM(isums.shape, F32),
            pltpu.VMEM((1, features), F32),
            pltpu.VMEM((4 * CAP, features), BF16),
            pltpu.VMEM((seq, features), BF16),
            dma((10,)),
            dma((4,)),
            dma((4,)),
        ],
        compiler_params=pltpu.CompilerParams(vmem_limit_bytes=60 * 1024 * 1024),
        name="splice",
    )(
        image_grids.transpose(1, 2, 0),
        routing.T,
        text_embeds,
        img,
        tsums,
        isums,
        final_gain.reshape(1, -1),
    )


def solution(mesh):
    placed = (
        P("dp", None),
        P(),
        P(),
        P(None, "tensor"),
        P("tensor"),
        P("tensor", "dp"),
        P("tensor"),
        P("dp", "tensor"),
        P("tensor"),
        P(),
        P(),
    )
    return jax.shard_map(
        per_device,
        mesh=mesh,
        in_specs=placed,
        out_specs=(P("dp", "tensor"), P("dp", "tensor")),
        check_vma=False,
    )
```

```python
import functools

import jax
import jax.numpy as jnp
from jax import lax
from jax.experimental import pallas as pl
from jax.experimental.pallas import tpu as pltpu
from jax.sharding import PartitionSpec as P

MESH = pl.DeviceIdType.MESH
F32 = jnp.float32
BF16 = jnp.bfloat16
SHARDS = 32
CAP = 64
D = 8192
CH = 256
NCH = 5
HEADS = (128, 192)
SQRT_HALF = 0.7071067811865476


def wait_for(ref, sem):
    pltpu.make_async_copy(ref, ref, sem).wait()


def send(src, dst, send_sem, recv_sem, device):
    pltpu.make_async_remote_copy(
        src_ref=src,
        dst_ref=dst,
        send_sem=send_sem,
        recv_sem=recv_sem,
        device_id=device,
        device_id_type=MESH,
    ).start()


def loop(name, count, step):
    with jax.named_scope(name):
        lax.fori_loop(0, count, step, 0)


def row_squares(values):
    values = values[:, :128] + values[:, 128:]
    ones = jnp.ones((8, values.shape[1]), F32)
    return lax.dot_general(
        ones,
        values,
        (((1,), (1,)), ((), ())),
        precision=lax.Precision.HIGHEST,
        preferred_element_type=F32,
    )


def merge_kernel(
    routing_hbm,
    pat_hbm,
    gain_hbm,
    nbias_hbm,
    w1_hbm,
    b1_hbm,
    w2_hbm,
    b2_hbm,
    text_hbm,
    img_out,
    tsums_out,
    isums_out,
    routing_ref,
    gain_ref,
    nbias_ref,
    b1_ref,
    b2_ref,
    pat,
    w1,
    nbuf,
    mer,
    hid,
    wbuf,
    stage,
    text,
    dsend,
    drecv,
    xsend,
    xrecv,
    fbuf,
    obuf,
    img,
    tbuf,
    ibuf,
    lsem,
    s_small,
    s0,
    s_first,
    s_stage,
    s_swap,
    s_w,
    s_p,
    s_p0,
    s_e,
    s_h,
    s_d,
    s_x,
    s_i,
    s_t,
    s_s,
    r_om,
    r_op,
    r_p,
    r_fm,
    r_fp,
    r_pm,
    r_pp,
    r_p2,
    r_h1,
    r_h2,
    r_h3,
    r_d,
    r_x,
    r_i,
    r_t,
    r_s,
):
    d = lax.axis_index("dp")
    t = lax.axis_index("tensor")
    z = lax.div(d, 8)
    y = lax.rem(lax.div(d, 2), 4)
    xl = lax.rem(d, 2)
    xh = lax.div(t, 2)
    c = lax.rem(t, 2)
    zp = lax.rem(z + 1, 4)
    zm = lax.rem(z + 3, 4)
    zo = lax.rem(z + 2, 4)
    yb = y + 1 - 2 * lax.rem(y, 2)
    q = xl + xh - 2 * xl * xh
    dev_zp = (zp * 8 + y * 2 + xl, t)
    dev_zm = (zm * 8 + y * 2 + xl, t)
    dev_ya = (z * 8 + (3 - y) * 2 + xl, t)
    dev_yb = (z * 8 + yb * 2 + xl, t)
    dev_x = (z * 8 + y * 2 + 1 - xl, t)
    dev_cut = (z * 8 + y * 2 + 1 - xl, (1 - xh) * 2 + c)
    dev_core = (d, xh * 2 + 1 - c)

    @pl.when(xh == 0)
    def _():
        pltpu.make_async_copy(w2_hbm, wbuf.at[z * 2], s_stage).start()

    @pl.when(xh == 1)
    def _():
        pltpu.make_async_copy(w2_hbm, stage, s_stage).start()

    pltpu.make_async_copy(pat_hbm, pat, lsem.at[NCH]).start()

    small = [
        pltpu.make_async_copy(src, dst, s_small.at[i])
        for i, (src, dst) in enumerate(
            (
                (routing_hbm, routing_ref),
                (gain_hbm, gain_ref),
                (nbias_hbm, nbias_ref),
                (b1_hbm, b1_ref),
                (b2_hbm, b2_ref),
            )
        )
    ]
    for copy in small:
        copy.start()

    barrier = pltpu.get_barrier_semaphore()
    base = d - lax.rem(d, 4)

    def greet(device):
        pl.semaphore_signal(barrier, inc=1, device_id=device, device_id_type=MESH)

    for o in range(-4, 8):
        other = lax.rem(base + o + SHARDS, SHARDS)

        @pl.when(other != d)
        def _():
            greet((other, t))

    greet(dev_zp)
    greet(dev_zm)
    greet(dev_cut)
    for i in range(1, 4):
        greet((d, lax.rem(t + i, 4)))

    for copy in small:
        copy.wait()

    width = pat.shape[1]
    gain = gain_ref[...].reshape(1, width)
    nbias = nbias_ref[...].reshape(1, width)

    def norm_pair(pair, carry):
        for u in range(2):
            norm_step(pair * 2 + u, nbuf.at[u])
        return carry

    def norm_step(step, nbuf):
        slot = lax.div(step, 4)
        part = lax.rem(step, 4)
        values = jnp.zeros((64, width), BF16)
        for b in range(4):
            start = pl.multiple_of(b * (4 * CAP) + part * 64, 64)
            chosen = (routing_ref[b, d] == slot).astype(F32).astype(BF16)
            values = values + pat[pl.ds(start, 64), :] * chosen
        values = values.astype(F32)
        centered = values - jnp.mean(values, axis=-1, keepdims=True)
        variance = jnp.mean(centered * centered, axis=-1, keepdims=True)
        normed = centered * lax.rsqrt(variance + 1e-06) * gain + nbias
        row = pl.multiple_of(step * 16, 16)
        for i in range(width // 128):
            nbuf[i] = normed[:, i * 128 : (i + 1) * 128]
        for j in range(4):
            for i in range(width // 128):
                mer[pl.ds(row, 16), j * width + i * 128 : j * width + (i + 1) * 128] = (
                    nbuf[i, pl.ds(j, 16, stride=4), :].astype(BF16)
                )

    with jax.named_scope("patches_in"):
        wait_for(pat, lsem.at[NCH])
    for n in range(NCH):
        pltpu.make_async_copy(
            w1_hbm.at[:, pl.ds(n * CH, CH)], w1.at[n], lsem.at[n]
        ).start()
    with jax.named_scope("norm_first"):
        lax.fori_loop(0, 2, norm_pair, 0)
    with jax.named_scope("greeting"):
        pl.semaphore_wait(barrier, 17)

    def own_send(kc, part=pl.ds(0, CH)):
        block = wbuf.at[z * 2, kc, part]
        send(block, block, s_w, r_om.at[kc], dev_zp)
        send(block, block, s_w, r_op.at[kc], dev_zm)
        send(block, wbuf.at[z * 2 + 1, kc, part], s_w, r_p.at[kc], dev_ya)

    with jax.named_scope("second_in"):
        wait_for(stage, s_stage)

    halves = (pl.ds(0, CH // 2), pl.ds(CH // 2, CH // 2))

    def swapped_half(half):
        with jax.named_scope("swapped"):
            wait_for(wbuf.at[z * 2, 0, halves[half]], s_first.at[half])
        own_send(0, halves[half])

    def swapped_send(kc):
        with jax.named_scope("swapped"):
            wait_for(wbuf.at[z * 2, kc], s0.at[kc])
        own_send(kc)

    @pl.when(xh == 1)
    def _():
        for half in range(2):
            send(
                stage.at[0, halves[half]],
                wbuf.at[z * 2, 0, halves[half]],
                s_swap,
                s_first.at[half],
                dev_x,
            )
        for kc in range(1, NCH):
            send(stage.at[kc], wbuf.at[z * 2, kc], s_swap, s0.at[kc], dev_x)

    @pl.when(xh == 0)
    def _():
        for kc in range(3):
            own_send(kc)

    with jax.named_scope("norm_rest"):
        lax.fori_loop(2, 8, norm_pair, 0)

    @pl.when(xh == 0)
    def _():
        own_send(3)
        own_send(4)

    @pl.when(xh == 1)
    def _():
        swapped_half(0)

    def hidden_step(n, carry):
        wait_for(w1.at[n], lsem.at[n])
        value = jnp.dot(mer[...], w1[n], preferred_element_type=F32)
        value = value + b1_ref[pl.ds(pl.multiple_of(n * CH, CH), CH)].reshape(1, CH)
        value = 0.5 * value * (1.0 + lax.erf(value * SQRT_HALF))
        hid[0, n] = value.astype(BF16)
        send(hid.at[0, n], hid.at[1, n], s_h, r_h1.at[n], dev_x)
        send(hid.at[0, n], hid.at[2, n], s_h, r_h2.at[n], dev_yb)

        @pl.when((xh == 1) & (n == 0))
        def _():
            swapped_half(1)

        @pl.when((xh == 1) & ((n == 2) | (n == 4)))
        def _():
            swapped_send(lax.div(n, 2))

        return carry

    loop("hidden_step", NCH, hidden_step)

    pltpu.make_async_copy(text_hbm, text, lsem.at[NCH + 1]).start()

    def far(kc):
        wait_for(wbuf.at[zm * 2, kc], r_om.at[kc])
        upper = wbuf.at[zm * 2, kc, pl.ds(0, CH // 2)]
        send(upper, upper, s_w, r_fm.at[kc], dev_zp)
        wait_for(wbuf.at[zp * 2, kc], r_op.at[kc])
        under = wbuf.at[zp * 2, kc, pl.ds(CH // 2, CH // 2)]
        send(under, under, s_w, r_fp.at[kc], dev_zm)

    def late_own(kc):
        @pl.when(xh == 1)
        def _():
            swapped_send(kc)

    def pair(kc):
        block = wbuf.at[z * 2 + 1, kc]
        wait_for(block, r_p.at[kc])
        if kc > 0:
            send(block, block, s_p, r_pm, dev_zp)
            send(block, block, s_p, r_pp, dev_zm)
        else:
            @pl.when(lax.div(z, 2) == xh)
            def _():
                send(block, block, s_p0, r_pm, dev_zp)
                send(block, block, s_p0, r_pp, dev_zm)

    def pair_first():
        for near, sem in ((zm, r_pm), (zp, r_pp)):

            @pl.when(lax.div(near, 2) != xh)
            def _():
                send(wbuf.at[near * 2, 0], wbuf.at[near * 2 + 1, 0], s_e, sem, dev_ya)

    def rows_x(n):
        wait_for(hid.at[1, n], r_h1.at[n])
        for half in range(2):

            @pl.when(xh == half)
            def _():
                top = pl.ds(0, HEADS[half])
                send(hid.at[1, n, top], hid.at[3, n, top], s_h, r_h3, dev_yb)

    def rows_y(n):
        wait_for(hid.at[2, n], r_h2.at[n])
        for half in range(2):

            @pl.when(xh == half)
            def _():
                rest = pl.ds(HEADS[half], CH - HEADS[half])
                send(hid.at[2, n, rest], hid.at[3, n, rest], s_h, r_h3, dev_x)

    def across_y(n):
        wait_for(wbuf.at[zo * 2, n, pl.ds(0, CH // 2)], r_fm.at[n])
        wait_for(wbuf.at[zo * 2, n, pl.ds(CH // 2, CH // 2)], r_fp.at[n])
        send(wbuf.at[zo * 2, n], wbuf.at[zo * 2 + 1, n], s_w, r_p2, dev_ya)

    def tile(rows, group, p):
        count = len(rows) * CH
        left = jnp.concatenate(
            [hid[rows[0] : rows[-1] + 1, n].reshape(count, CH) for n in range(NCH)],
            axis=1,
        )
        right = wbuf[group * 2 + p].reshape(NCH * CH, CH)
        return jnp.dot(left, right, preferred_element_type=F32)

    swap = lax.rem(z + c, 2)

    def pick(a, b, first):
        return a * first + b * (1 - first)

    def column_of(p):
        return (y + p * (3 - 2 * y)) * 2 + q

    def tiles(same, opposite):
        if same is None or opposite is None:
            to_z, to_p = my_z, my_p = opposite if same is None else same
        else:
            to_z = pick(same[0], opposite[0], swap)
            to_p = pick(same[1], opposite[1], swap)
            my_z = pick(opposite[0], same[0], swap)
            my_p = pick(opposite[1], same[1], swap)
        to_half = lax.rem(lax.div(to_z, 2) + xh + 1, 2)
        my_half = lax.rem(lax.div(my_z, 2) + xh + 1, 2)

        def give(rows):
            value = tile(rows, to_z, to_p).astype(BF16)

            def out():
                for i, r in enumerate(rows):
                    dsend[to_half, to_p, r] = value[i * CH : (i + 1) * CH]
                    send(
                        dsend.at[to_half, to_p, r],
                        drecv.at[to_half, to_p, r],
                        s_d,
                        r_d.at[to_half * 8 + to_p * 4 + r],
                        dev_core,
                    )

            return out

        def take(rows):
            value = tile(rows, my_z, my_p)

            def out():
                for i, r in enumerate(rows):
                    wait_for(
                        drecv.at[my_half, my_p, r], r_d.at[my_half * 8 + my_p * 4 + r]
                    )
                    mine = value[i * CH : (i + 1) * CH]
                    mine = mine + drecv[my_half, my_p, r].astype(F32)

                    @pl.when(my_half == 0)
                    def _():
                        xsend[my_p, r] = mine.astype(BF16)
                        there = r + 1 - 2 * (r % 2)
                        send(
                            xsend.at[my_p, r],
                            xrecv.at[my_p, there],
                            s_x,
                            r_x.at[my_p * 4 + there],
                            dev_cut,
                        )

                    @pl.when(my_half == 1)
                    def _():
                        column = pl.multiple_of(column_of(my_p) * CH, CH)
                        fbuf[my_p, r] = mine + b2_ref[:, pl.ds(column, CH)]

            return out

        return give, take

    near_a = tiles((z, 0), (zm, 0))
    near_b = tiles((z, 1), (zp, 0))
    middle = tiles((zo, 0), None)
    up = lax.rem(lax.div(zp, 2) + xh, 2)
    far_a = tiles((zo, 1), None)
    far_b = tiles(None, (pick(zp, zm, up), 1))
    far_c = tiles(None, (pick(zm, zp, up), 1))

    def give_near(r):
        with jax.named_scope(f"give_near{r}"):
            outs = [near_a[0]([r]), near_b[0]([r])]
            for out in outs:
                out()

    def take_near(r):
        with jax.named_scope(f"take_near{r}"):
            outs = [near_a[1]([r]), near_b[1]([r])]
            for out in outs:
                out()

    def run_single(name, steps, mine, rows):
        with jax.named_scope(name):

            @pl.when(swap != mine)
            def _():
                steps[0](rows)()

            @pl.when(swap == mine)
            def _():
                steps[1](rows)()

    def text_step(i, carry):
        rows = pl.ds(pl.multiple_of(i * CH, CH), CH)
        total = jnp.zeros((CH, CH), F32)
        for j in range(8):
            values = text[rows, j * CH : (j + 1) * CH].astype(F32)
            total = total + values * values
        tbuf[:, rows] = row_squares(total)
        return carry

    def share(buf, result, own_sem, send_sems, recv_sems):
        pltpu.make_async_copy(buf, result.at[t], own_sem).start()
        for i in range(1, 4):
            send(
                buf,
                result.at[t],
                send_sems.at[i - 1],
                recv_sems.at[i - 1],
                (d, lax.rem(t + i, 4)),
            )

    def step(label, work, *args):
        with jax.named_scope(label):
            work(*args)

    def target(r, k):
        row_y = y + lax.div(r, 2) * (yb - y)
        row_x = xl + lax.rem(r, 2) * (1 - 2 * xl)
        return lax.rem(z * 8 + row_y * 2 + row_x + k, SHARDS)

    def pieces(p, r, k):
        rows = pl.ds(k * CAP, CAP)
        return obuf.at[p, r, rows], img.at[column_of(p), rows]

    def finish(p, r):
        with jax.named_scope(f"finish{p}{r}"):
            wait_for(xrecv.at[p, r], r_x.at[p * 4 + r])
            obuf[p, r] = (fbuf[p, r] + xrecv[p, r].astype(F32)).astype(BF16)
            for k in range(4):
                e = target(r, k)
                src, dst = pieces(p, r, k)

                @pl.when(e == d)
                def _():
                    pltpu.make_async_copy(src, dst, r_i).start()

                @pl.when((e != d) & (lax.div(e, 4) == lax.div(d, 4)))
                def _():
                    send(src, dst, s_i.at[p * 16 + r * 4 + k], r_i, (e, t))

    def onward(p, r):
        for k in range(1, 4):
            e = target(r, k)
            src, dst = pieces(p, r, k)

            @pl.when(lax.div(e, 4) != lax.div(d, 4))
            def _():
                send(src, dst, s_i.at[p * 16 + r * 4 + k], r_i, (e, t))

    def on_side(side, *work):
        @pl.when(xh == side)
        def _():
            for do, p, rows in work:
                for r in rows:
                    do(p, r)

    step("far0", far, 0)
    step("rows_y0", rows_y, 0)
    late_own(3)
    step("far1", far, 1)
    step("rows_y1", rows_y, 1)
    late_own(4)
    with jax.named_scope("text_in"):
        wait_for(text, lsem.at[NCH + 1])
    loop("text_step", 2, text_step)
    share(tbuf, tsums_out, lsem.at[2], s_t, r_t)
    step("far2", far, 2)
    step("rows_y2", rows_y, 2)
    step("rows_x0", rows_x, 0)
    step("across_y0", across_y, 0)
    step("far3", far, 3)
    step("rows_y3", rows_y, 3)
    step("across_y1", across_y, 1)
    step("rows_x1", rows_x, 1)
    step("rows_y4", rows_y, 4)
    step("far4", far, 4)
    for kc in range(NCH):
        step(f"pair{kc}", pair, kc)
    give_near(0)
    step("rows_x2", rows_x, 2)
    step("across_y2", across_y, 2)
    take_near(0)
    give_near(2)
    step("across_y3", across_y, 3)
    step("rows_x3", rows_x, 3)
    take_near(2)
    step("across_y4", across_y, 4)
    pair_first()
    run_single("middle", middle, 0, [0])
    step("rows_x4", rows_x, 4)
    give_near(1)
    run_single("middle", middle, 0, [1, 2])
    take_near(1)
    with jax.named_scope("diagonal"):
        wait_for(hid.at[3], r_h3)
    on_side(1, (finish, 0, (1, 0)))
    give_near(3)
    run_single("middle3", middle, 0, [3])
    take_near(3)

    @pl.when((xh == 0) & (t != zo))
    def _():
        finish(0, 1)

    on_side(1, (finish, 0, (3, 2)))
    every = [0, 1, 2, 3]
    with jax.named_scope("pair_blocks_o"):
        wait_for(wbuf.at[zo * 2 + 1], r_p2)
    run_single("far_a", far_a, 0, every)

    @pl.when((xh == 0) & (t == zo))
    def _():
        finish(0, 1)

    on_side(0, (onward, 0, (1,)))
    on_side(1, (onward, 0, (1, 0, 3, 2)))
    with jax.named_scope("pair_blocks"):
        wait_for(wbuf.at[zm * 2 + 1], r_pm)
        wait_for(wbuf.at[zp * 2 + 1], r_pp)
    run_single("far_b", far_b, 1, every)
    on_side(0, (finish, 0, (3,)), (onward, 0, (3,)))
    run_single("far_c", far_c, 1, every)
    on_side(0, (finish, 0, (0,)), (onward, 0, (0,)))
    on_side(0, (finish, 0, (2,)), (onward, 0, (2,)))
    for r in (1, 0, 3, 2):
        finish(1, r)
        onward(1, r)

    with jax.named_scope("image_in"):
        wait_for(img, r_i)
    img_copy = pltpu.make_async_copy(img, img_out, lsem.at[0])
    img_copy.start()
    total = jnp.zeros((CH, CH), F32)
    for b in range(8):
        values = img[b].astype(F32)
        total = total + values * values
    ibuf[...] = row_squares(total)
    share(ibuf, isums_out, lsem.at[1], s_s, r_s)
    for i in range(1, 4):
        wait_for(tsums_out.at[lax.rem(t + 4 - i, 4)], r_t.at[i - 1])
    wait_for(tbuf, lsem.at[2])
    with jax.named_scope("sums_in"):
        for i in range(1, 4):
            wait_for(isums_out.at[lax.rem(t + 4 - i, 4)], r_s.at[i - 1])
    wait_for(ibuf, lsem.at[1])

    wait_for(wbuf.at[pl.ds(0, 5)], s_w)
    wait_for(wbuf.at[pl.ds(0, 2), pl.ds(0, 4)], s_p)
    wait_for(wbuf.at[0, 0], s_e)

    @pl.when(lax.div(z, 2) == xh)
    def _():
        wait_for(wbuf.at[pl.ds(0, 2), 0], s_p0)

    @pl.when(xh == 1)
    def _():
        wait_for(wbuf.at[0], s_swap)

    wait_for(hid.at[pl.ds(0, 3)], s_h)
    wait_for(dsend, s_d)
    wait_for(xsend, s_x)
    for p in range(2):

        def drain(r, carry):
            for k in range(4):
                src, _unused = pieces(p, r, k)

                @pl.when(target(r, k) != d)
                def _():
                    wait_for(src, s_i.at[p * 16 + r * 4 + k])

            return carry

        loop("drain", 4, drain)
    for i in range(1, 4):
        wait_for(tbuf, s_t.at[i - 1])
        wait_for(ibuf, s_s.at[i - 1])
    img_copy.wait()


def splice_kernel(
    grids_hbm,
    routing_hbm,
    text_hbm,
    img_hbm,
    tsums_hbm,
    isums_hbm,
    gain_hbm,
    emb_hbm,
    out_hbm,
    grids_ref,
    routing_ref,
    text,
    img,
    tsums,
    isums,
    gain,
    emb,
    out,
    in_sem,
    emb_sem,
    out_sem,
):
    rows = 128
    images = 4 * CAP
    steps = text.shape[0] // rows
    first = images // rows

    def part(ref, i):
        return ref.at[pl.ds(i * rows, rows)]

    small = [
        pltpu.make_async_copy(tsums_hbm, tsums, in_sem.at[steps]),
        pltpu.make_async_copy(isums_hbm, isums, in_sem.at[steps + 1]),
        pltpu.make_async_copy(gain_hbm, gain, in_sem.at[steps + 2]),
    ]
    whole = pltpu.make_async_copy(img_hbm, img, in_sem.at[steps + 3])
    order = list(range(first, steps)) + list(range(first))
    loads = {
        i: pltpu.make_async_copy(part(text_hbm, i), part(text, i), in_sem.at[i])
        for i in order
    }
    for copy in small[:1] + small[2:]:
        copy.start()
    for i in order[: steps - first]:
        loads[i].start()
    whole.start()
    small[1].start()
    tables = [
        pltpu.make_async_copy(grids_hbm, grids_ref, in_sem.at[steps + 4]),
        pltpu.make_async_copy(routing_hbm, routing_ref, in_sem.at[steps + 5]),
    ]
    for copy in tables:
        copy.start()
    for i in order[steps - first :]:
        loads[i].start()

    d = lax.axis_index("dp")
    for copy in tables:
        copy.wait()
    starts = []
    total = jnp.int32(0)
    for k in range(4):
        s = lax.rem(d + SHARDS - k, SHARDS)
        count = jnp.int32(0)
        for b in range(4):
            size = grids_ref[b, 0, s] * grids_ref[b, 1, s]
            count = count + jnp.where(routing_ref[b, s] == k, size, 0)
        starts.append(total)
        total = total + count

    def picked(sums_ref, index):
        sums = sums_ref[0] + sums_ref[1] + sums_ref[2] + sums_ref[3]
        sums = sums[0:1, :]
        lanes = lax.broadcasted_iota(jnp.int32, (rows, sums.shape[1]), 1)
        return jnp.sum(jnp.where(lanes == index, sums, 0.0), axis=-1, keepdims=True)

    copies = []
    for copy in small[:1] + small[2:]:
        copy.wait()
    for i in order:
        position = i * rows + lax.broadcasted_iota(jnp.int32, (rows, 1), 0)
        square = picked(tsums, position)
        loads[i].wait()
        if i >= first:
            copies.append(
                pltpu.make_async_copy(part(text, i), part(emb_hbm, i), emb_sem.at[i])
            )
            copies[-1].start()
            scale = lax.rsqrt(square / D + 1e-06)
        else:
            if i == 0:
                whole.wait()
                small[1].wait()
            source = position
            for k in range(1, 4):
                shift = k * CAP - starts[k]
                if k > 1:
                    shift = shift - ((k - 1) * CAP - starts[k - 1])
                source = source + jnp.where(position >= starts[k], shift, 0)
            live = position < total
            square = jnp.where(live, picked(isums, source), square)
            scale = lax.rsqrt(square / D + 1e-06)
            picks = jnp.where(
                lax.broadcasted_iota(jnp.int32, (rows, images), 1) == source, 1.0, 0.0
            ).astype(BF16)
        here = slice(i * rows, (i + 1) * rows)
        for b in range(img.shape[0]):
            cols = slice(b * CH, (b + 1) * CH)
            value = text[here, cols].astype(F32)
            if i < first:
                taken = jnp.dot(picks, img[b], preferred_element_type=F32)
                value = jnp.where(live, taken, value)
                emb[here, cols] = value.astype(BF16)
            out[here, cols] = (value * scale * gain[:, cols]).astype(BF16)
        if i < first:
            copies.append(
                pltpu.make_async_copy(part(emb, i), part(emb_hbm, i), emb_sem.at[i])
            )
            copies[-1].start()
        copies.append(
            pltpu.make_async_copy(part(out, i), part(out_hbm, i), out_sem.at[i])
        )
        copies[-1].start()
    for copy in copies:
        copy.wait()


def per_device(
    patches,
    norm_gain,
    norm_bias,
    first_weight,
    first_bias,
    second_weight,
    second_bias,
    text_embeds,
    final_gain,
    image_grids,
    routing,
):
    seq, features = text_embeds.shape
    width = patches.shape[1]
    anywhere = pl.BlockSpec(memory_space=pl.ANY)
    dma = pltpu.SemaphoreType.DMA
    img, tsums, isums = pl.pallas_call(
        merge_kernel,
        out_shape=(
            jax.ShapeDtypeStruct((8, CH, CH), BF16),
            jax.ShapeDtypeStruct((4, 8, seq), F32),
            jax.ShapeDtypeStruct((4, 8, CH), F32),
        ),
        in_specs=[pl.BlockSpec(memory_space=pltpu.HBM)] * 9,
        out_specs=(anywhere, anywhere, anywhere),
        scratch_shapes=[
            pltpu.SMEM(routing.T.shape, jnp.int32),
            pltpu.VMEM(norm_gain.shape, F32),
            pltpu.VMEM(norm_bias.shape, F32),
            pltpu.VMEM(first_bias.shape, F32),
            pltpu.VMEM((1, second_bias.shape[0]), F32),
            pltpu.VMEM(patches.shape, BF16),
            pltpu.VMEM((NCH, first_weight.shape[0], CH), BF16),
            pltpu.VMEM((2, width // 128, 64, 128), F32),
            pltpu.VMEM((CH, 4 * width), BF16),
            pltpu.VMEM((4, NCH, CH, CH), BF16),
            pltpu.VMEM((8, NCH, CH, CH), BF16),
            pltpu.VMEM((NCH, CH, CH), BF16),
            pltpu.VMEM((seq, features), BF16),
            pltpu.VMEM((2, 2, 4, CH, CH), BF16),
            pltpu.VMEM((2, 2, 4, CH, CH), BF16),
            pltpu.VMEM((2, 4, CH, CH), BF16),
            pltpu.VMEM((2, 4, CH, CH), BF16),
            pltpu.VMEM((2, 4, CH, CH), F32),
            pltpu.VMEM((2, 4, CH, CH), BF16),
            pltpu.VMEM((8, CH, CH), BF16),
            pltpu.VMEM((8, seq), F32),
            pltpu.VMEM((8, CH), F32),
            dma((NCH + 2,)),
            dma((5,)),
            dma((NCH,)),
            dma((2,)),
            dma,
            dma,
            dma,
            dma,
            dma,
            dma,
            dma,
            dma,
            dma,
            dma((32,)),
            dma((3,)),
            dma((3,)),
            dma((NCH,)),
            dma((NCH,)),
            dma((NCH,)),
            dma((NCH,)),
            dma((NCH,)),
            dma,
            dma,
            dma,
            dma((NCH,)),
            dma((NCH,)),
            dma,
            dma((16,)),
            dma((8,)),
            dma,
            dma((3,)),
            dma((3,)),
        ],
        compiler_params=pltpu.CompilerParams(
            collective_id=0, has_side_effects=True, vmem_limit_bytes=60 * 1024 * 1024
        ),
        name="merge",
    )(
        routing.T,
        patches,
        norm_gain,
        norm_bias,
        first_weight,
        first_bias,
        second_weight.reshape(NCH, CH, CH),
        second_bias.reshape(1, -1),
        text_embeds,
    )
    return pl.pallas_call(
        splice_kernel,
        out_shape=(
            jax.ShapeDtypeStruct((seq, features), BF16),
            jax.ShapeDtypeStruct((seq, features), BF16),
        ),
        in_specs=[anywhere] * 7,
        out_specs=(anywhere, anywhere),
        scratch_shapes=[
            pltpu.SMEM((image_grids.shape[1], 2, SHARDS), jnp.int32),
            pltpu.SMEM(routing.T.shape, jnp.int32),
            pltpu.VMEM((seq, features), BF16),
            pltpu.VMEM(img.shape, BF16),
            pltpu.VMEM(tsums.shape, F32),
            pltpu.VMEM(isums.shape, F32),
            pltpu.VMEM((1, features), F32),
            pltpu.VMEM((4 * CAP, features), BF16),
            pltpu.VMEM((seq, features), BF16),
            dma((10,)),
            dma((4,)),
            dma((4,)),
        ],
        compiler_params=pltpu.CompilerParams(vmem_limit_bytes=60 * 1024 * 1024),
        name="splice",
    )(
        image_grids.transpose(1, 2, 0),
        routing.T,
        text_embeds,
        img,
        tsums,
        isums,
        final_gain.reshape(1, -1),
    )


def solution(mesh):
    placed = (
        P("dp", None),
        P(),
        P(),
        P(None, "tensor"),
        P("tensor"),
        P("tensor", "dp"),
        P("tensor"),
        P("dp", "tensor"),
        P("tensor"),
        P(),
        P(),
    )
    return jax.shard_map(
        per_device,
        mesh=mesh,
        in_specs=placed,
        out_specs=(P("dp", "tensor"), P("dp", "tensor")),
        check_vma=False,
    )
```
